8 devices in a mesh: rep: 1 (over z), data: 8 (over y, x, core).
Axes of the slice: x: 2, y: 2, z: 1, core: 2. Of those that a mesh axis runs over, the one named last changes fastest.
Arguments:
- x: bfloat16 [1024, 2048], P(('rep', 'data'))
- adapter_id: int32 [1024], P(('rep', 'data'))
- dout: bfloat16 [1024, 2048], P(('rep', 'data'))
- w_gate: bfloat16 [2048, 8192], replicated
- w_up: bfloat16 [2048, 8192], replicated
- w_down: bfloat16 [8192, 2048], replicated
- a_gate: bfloat16 [256, 2048, 16], P('data')
- b_gate: bfloat16 [256, 16, 8192], P('data')
- a_up: bfloat16 [256, 2048, 16], P('data')
- b_up: bfloat16 [256, 16, 8192], P('data')
- a_down: bfloat16 [256, 8192, 16], P('data')
- b_down: bfloat16 [256, 16, 2048], P('data')
Outputs:
- output 1: bfloat16 [1024, 2048], P(('rep', 'data'))
- output 2: bfloat16 [1024, 2048], P(('rep', 'data'))
- output 3: float32 [256, 2048, 16], P(('rep', 'data'))
- output 4: float32 [256, 16, 8192], P(('rep', 'data'))
- output 5: float32 [256, 2048, 16], P(('rep', 'data'))
- output 6: float32 [256, 16, 8192], P(('rep', 'data'))
- output 7: float32 [256, 8192, 16], P(('rep', 'data'))
- output 8: float32 [256, 16, 2048], P(('rep', 'data'))
All inputs are finite; a program needn't handle non-finite values.
Results may differ from the reference program's by a relative error of at most 0.00149.
Values are sent between devices in bfloat16 or wider.
A program may use at most 1 GiB of HBM per device.

```python
import jax
import jax.numpy as jnp
from jax import lax

TOKENS = 128
ADAPTERS = 32
MODEL_DIM = 2048
HIDDEN_DIM = 8192
LORA_RANK = 16
GROUP_SIZE = 8
CAPACITY = 48
LORA_ALPHA = 32
BLOCK_ROWS = 32

PART_TOKENS = TOKENS * GROUP_SIZE
NUM_ADAPTERS = ADAPTERS * GROUP_SIZE
LORA_SCALE = LORA_ALPHA / LORA_RANK


def draw_ids(rand_key):
    key_hot, key_off, key_shift, key_perm = jax.random.split(rand_key, 4)
    hot_owner = jax.random.randint(key_hot, (), 0, GROUP_SIZE)
    start_offset = jax.random.randint(key_off, (), 0, GROUP_SIZE - 1)
    owner_shift = jax.random.randint(key_shift, (GROUP_SIZE,), 0, ADAPTERS)
    spare_rows = TOKENS - CAPACITY
    source_dev = jnp.arange(GROUP_SIZE)[:, None]
    column_idx = jnp.arange(TOKENS)[None, :]
    hot_mask = column_idx < CAPACITY
    hot_local = (source_dev * CAPACITY + column_idx + owner_shift[hot_owner]) % ADAPTERS
    flat_index = start_offset + source_dev * spare_rows + column_idx - CAPACITY
    other_owner = (hot_owner + 1 + flat_index % (GROUP_SIZE - 1)) % GROUP_SIZE
    visit_count = flat_index // (GROUP_SIZE - 1)
    other_local = (visit_count + owner_shift[other_owner]) % ADAPTERS
    owner_ids = jnp.where(hot_mask, hot_owner, other_owner)
    local_ids = jnp.where(hot_mask, hot_local, other_local)
    id_table = owner_ids * ADAPTERS + local_ids
    perm_keys = jax.random.split(key_perm, GROUP_SIZE)
    perm_rows = jax.vmap(lambda perm_key: jax.random.permutation(perm_key, TOKENS))(perm_keys)
    id_table = jnp.take_along_axis(id_table, perm_rows, axis=1)
    return id_table.reshape(-1).astype(jnp.int32)


def normal_bf16(key_one, arr_shape, spread):
    return (jax.random.normal(key_one, arr_shape, jnp.float32) * spread).astype(jnp.bfloat16)


def setup_inputs(seed: int = 0, part: int = 0) -> dict:
    base_key = jax.random.key(seed)
    part_key = jax.random.fold_in(base_key, part)
    shared_keys = jax.random.split(base_key, 9)
    part_keys = jax.random.split(part_key, 3)
    b_std = 0.3 * LORA_RANK ** -0.5 / LORA_SCALE
    d_std = MODEL_DIM ** -0.5
    f_std = HIDDEN_DIM ** -0.5
    return {
        'x': normal_bf16(part_keys[0], (PART_TOKENS, MODEL_DIM), 1.0),
        'adapter_id': draw_ids(part_keys[1]),
        'dout': normal_bf16(part_keys[2], (PART_TOKENS, MODEL_DIM), 1.0),
        'w_gate': normal_bf16(shared_keys[0], (MODEL_DIM, HIDDEN_DIM), d_std),
        'w_up': normal_bf16(shared_keys[1], (MODEL_DIM, HIDDEN_DIM), d_std),
        'w_down': normal_bf16(shared_keys[2], (HIDDEN_DIM, MODEL_DIM), f_std),
        'a_gate': normal_bf16(shared_keys[3], (NUM_ADAPTERS, MODEL_DIM, LORA_RANK), d_std),
        'b_gate': normal_bf16(shared_keys[4], (NUM_ADAPTERS, LORA_RANK, HIDDEN_DIM), b_std),
        'a_up': normal_bf16(shared_keys[5], (NUM_ADAPTERS, MODEL_DIM, LORA_RANK), d_std),
        'b_up': normal_bf16(shared_keys[6], (NUM_ADAPTERS, LORA_RANK, HIDDEN_DIM), b_std),
        'a_down': normal_bf16(shared_keys[7], (NUM_ADAPTERS, HIDDEN_DIM, LORA_RANK), f_std),
        'b_down': normal_bf16(shared_keys[8], (NUM_ADAPTERS, LORA_RANK, MODEL_DIM), b_std),
    }


def bf16_cast(values):
    return values.astype(jnp.bfloat16).astype(jnp.float32)


def reference(x, adapter_id, dout, w_gate, w_up, w_down, a_gate, b_gate, a_up, b_up, a_down, b_down):
    gate_wt = w_gate.astype(jnp.float32)
    up_wt = w_up.astype(jnp.float32)
    down_wt = w_down.astype(jnp.float32)
    model_width = x.shape[1]
    num_blocks = x.shape[0] // BLOCK_ROWS

    def block_step(grad_sums, block_in):
        x_blk, id_blk, dy_blk = block_in
        x_rows = x_blk.astype(jnp.float32)
        dy_rows = dy_blk.astype(jnp.float32)
        ag_rows = a_gate[id_blk].astype(jnp.float32)
        bg_rows = b_gate[id_blk].astype(jnp.float32)
        au_rows = a_up[id_blk].astype(jnp.float32)
        bu_rows = b_up[id_blk].astype(jnp.float32)
        ad_rows = a_down[id_blk].astype(jnp.float32)
        bd_rows = b_down[id_blk].astype(jnp.float32)
        p_gate = bf16_cast(jnp.einsum('td,tdr->tr', x_rows, ag_rows))
        p_up = bf16_cast(jnp.einsum('td,tdr->tr', x_rows, au_rows))
        e_gate = bf16_cast(LORA_SCALE * jnp.einsum('tr,trf->tf', p_gate, bg_rows))
        e_up = bf16_cast(LORA_SCALE * jnp.einsum('tr,trf->tf', p_up, bu_rows))
        gate_pre = jnp.dot(x_rows, gate_wt) + e_gate
        up_pre = jnp.dot(x_rows, up_wt) + e_up
        gate_sig = jax.nn.sigmoid(gate_pre)
        gate_act = gate_pre * gate_sig
        hidden = bf16_cast(gate_act * up_pre)
        p_down = bf16_cast(jnp.einsum('tf,tfr->tr', hidden, ad_rows))
        e_down = bf16_cast(LORA_SCALE * jnp.einsum('tr,trd->td', p_down, bd_rows))
        out_blk = (x_rows + jnp.dot(hidden, down_wt) + e_down).astype(jnp.bfloat16)
        q_down = bf16_cast(LORA_SCALE * jnp.einsum('td,trd->tr', dy_rows, bd_rows))
        dh_lora = bf16_cast(jnp.einsum('tr,tfr->tf', q_down, ad_rows))
        d_hidden = jnp.einsum('td,fd->tf', dy_rows, down_wt) + dh_lora
        d_gate = bf16_cast(d_hidden * up_pre * gate_sig * (1.0 + gate_pre * (1.0 - gate_sig)))
        d_up = bf16_cast(d_hidden * gate_act)
        q_gate = bf16_cast(LORA_SCALE * jnp.einsum('tf,trf->tr', d_gate, bg_rows))
        q_up = bf16_cast(LORA_SCALE * jnp.einsum('tf,trf->tr', d_up, bu_rows))
        dx_lora = bf16_cast(jnp.einsum('tr,tdr->td', q_gate, ag_rows) + jnp.einsum('tr,tdr->td', q_up, au_rows))
        dx_blk = (dy_rows + jnp.einsum('tf,df->td', d_gate, gate_wt) + jnp.einsum('tf,df->td', d_up, up_wt) + dx_lora).astype(jnp.bfloat16)
        updates = (
            jnp.einsum('td,tr->tdr', x_rows, q_gate),
            LORA_SCALE * jnp.einsum('tr,tf->trf', p_gate, d_gate),
            jnp.einsum('td,tr->tdr', x_rows, q_up),
            LORA_SCALE * jnp.einsum('tr,tf->trf', p_up, d_up),
            jnp.einsum('tf,tr->tfr', hidden, q_down),
            LORA_SCALE * jnp.einsum('tr,td->trd', p_down, dy_rows),
        )
        new_sums = tuple(grad_acc.at[id_blk].add(grad_upd) for grad_acc, grad_upd in zip(grad_sums, updates))
        return new_sums, (out_blk, dx_blk)

    init_sums = tuple(jnp.zeros(weight.shape, jnp.float32) for weight in (a_gate, b_gate, a_up, b_up, a_down, b_down))
    blocks_in = (
        x.reshape(num_blocks, BLOCK_ROWS, model_width),
        adapter_id.reshape(num_blocks, BLOCK_ROWS),
        dout.reshape(num_blocks, BLOCK_ROWS, model_width),
    )
    grad_sums, (out_rows, dx_rows) = lax.scan(block_step, init_sums, blocks_in)
    return (out_rows.reshape(-1, model_width), dx_rows.reshape(-1, model_width), grad_sums[0], grad_sums[1], grad_sums[2], grad_sums[3], grad_sums[4], grad_sums[5])
```

```python
import jax
import jax.numpy as jnp
from jax import lax
from jax.sharding import PartitionSpec as P

LORA_ALPHA = 32


def mm(left, right, ldim=1, rdim=0):
    return lax.dot_general(left, right, (((ldim,), (rdim,)), ((), ())), preferred_element_type=jnp.float32)


def solution(mesh):
    group = mesh.shape['data']
    tok_spec = P(('rep', 'data'), None)
    id_spec = P(('rep', 'data'))
    full_spec = P(None, None)
    own_spec = P('data', None, None)
    grad_spec = P(('rep', 'data'), None, None)
    bf = jnp.bfloat16

    def device_fn(x_loc, ids_loc, dy_loc, w_gate, w_up, w_down, a_gate, b_gate, a_up, b_up, a_down, b_down):
        tokens, dim = x_loc.shape
        n_local, _, rank = a_gate.shape
        hidden = w_gate.shape[1]
        width = n_local * rank
        scale = LORA_ALPHA / rank
        cap = ((3 * tokens + 8 * group - 1) // (8 * group)) * 8
        rows = group * cap
        owner = ids_loc // n_local
        local = ids_loc % n_local
        before = (owner[:, None] == owner[None, :]) & (jnp.arange(tokens)[None, :] < jnp.arange(tokens)[:, None])
        slot = owner * cap + before.astype(jnp.int32).sum(axis=1)
        hit = jnp.arange(rows)[:, None] == slot[None, :]
        pack = hit.astype(bf)
        slot_ids = jnp.where(hit, local[None, :] + 1, 0).max(axis=1) - 1

        def exchange(arr):
            return lax.all_to_all(arr, 'data', 0, 0, tiled=True)

        ids = exchange(slot_ids)
        x = exchange(mm(pack, x_loc).astype(bf))
        dy = exchange(mm(pack, dy_loc).astype(bf))
        mask = ids[:, None] == (jnp.arange(width) // rank)[None, :]

        def keep(vals):
            return jnp.where(mask, vals, 0.0).astype(bf)

        def as_rows(weight):
            return jnp.swapaxes(weight, 1, 2).reshape(width, weight.shape[1])

        ag, au, ad = as_rows(a_gate), as_rows(a_up), as_rows(a_down)
        bg, bu, bd = b_gate.reshape(width, hidden), b_up.reshape(width, hidden), b_down.reshape(width, dim)
        pg = keep(mm(x, ag, 1, 1))
        pu = keep(mm(x, au, 1, 1))
        f32 = jnp.float32
        gate = mm(x, w_gate) + (scale * mm(pg, bg)).astype(bf).astype(f32)
        up = mm(x, w_up) + (scale * mm(pu, bu)).astype(bf).astype(f32)
        sig = jax.nn.sigmoid(gate)
        act = gate * sig
        h = (act * up).astype(bf)
        pd = keep(mm(h, ad, 1, 1))
        out = (x.astype(f32) + mm(h, w_down) + (scale * mm(pd, bd)).astype(bf).astype(f32)).astype(bf)
        qd = keep(scale * mm(dy, bd, 1, 1))
        dh = mm(dy, w_down, 1, 1) + mm(qd, ad).astype(bf).astype(f32)
        dg = (dh * up * sig * (1.0 + gate * (1.0 - sig))).astype(bf)
        du = (dh * act).astype(bf)
        qg = keep(scale * mm(dg, bg, 1, 1))
        qu = keep(scale * mm(du, bu, 1, 1))
        dxl = (mm(qg, ag) + mm(qu, au)).astype(bf)
        dx = (dy.astype(f32) + mm(dg, w_gate, 1, 1) + mm(du, w_up, 1, 1) + dxl.astype(f32)).astype(bf)

        def back(arr):
            return mm(pack, exchange(arr), 0, 0).astype(bf)

        def a_grad(q, src):
            return jnp.swapaxes(mm(q, src, 0, 0).reshape(n_local, rank, src.shape[1]), 1, 2)

        def b_grad(p, src):
            return (scale * mm(p, src, 0, 0)).reshape(n_local, rank, src.shape[1])

        return (back(out), back(dx), a_grad(qg, x), b_grad(pg, dg), a_grad(qu, x), b_grad(pu, du),
                a_grad(qd, h), b_grad(pd, dy))

    return jax.shard_map(
        device_fn,
        mesh=mesh,
        in_specs=(tok_spec, id_spec, tok_spec, full_spec, full_spec, full_spec) + (own_spec,) * 6,
        out_specs=(tok_spec, tok_spec) + (grad_spec,) * 6,
        check_vma=False,
    )
```

```python
import functools

import jax
import jax.numpy as jnp
from jax import lax
from jax.experimental import pallas as pl
from jax.experimental.pallas import tpu as pltpu
from jax.sharding import PartitionSpec as P

LORA_ALPHA = 32
TILE = 512
f32 = jnp.float32
bf = jnp.bfloat16


def mm(left, right, ldim=1, rdim=0):
    return lax.dot_general(left, right, (((ldim,), (rdim,)), ((), ())), preferred_element_type=f32)


def rounded(vals):
    return vals.astype(bf).astype(f32)


def keep(vals, ids, rank):
    cols = lax.div(lax.broadcasted_iota(jnp.int32, vals.shape, 1), jnp.int32(rank))
    return jnp.where(cols == ids, vals, 0.0).astype(bf)


def forward_body(rank, scale, ids, x, ag, au, bd, wg, wu, wd, bg, bu, ad, gate_o, up_o, out_o, pg_o, pu_o, pd_o, acc, pd_acc):
    step = pl.program_id(0)

    @pl.when(step == 0)
    def _():
        pg_o[...] = keep(mm(x[...], ag[...], 1, 1), ids[...], rank)
        pu_o[...] = keep(mm(x[...], au[...], 1, 1), ids[...], rank)
        acc[...] = jnp.zeros_like(acc)
        pd_acc[...] = jnp.zeros_like(pd_acc)

    gate = mm(x[...], wg[...]) + rounded(scale * mm(pg_o[...], bg[...]))
    up = mm(x[...], wu[...]) + rounded(scale * mm(pu_o[...], bu[...]))
    gate_o[...] = gate
    up_o[...] = up
    h = (gate * jax.nn.sigmoid(gate) * up).astype(bf)
    acc[...] += mm(h, wd[...])
    pd_acc[...] += mm(h, ad[...], 1, 1)

    @pl.when(step == pl.num_programs(0) - 1)
    def _():
        pd = keep(pd_acc[...], ids[...], rank)
        pd_o[...] = pd
        out_o[...] = (x[...].astype(f32) + acc[...] + rounded(scale * mm(pd, bd[...]))).astype(bf)


def backward_body(rank, scale, ids, dy, ag, au, bd, gate_r, up_r, wg, wu, wd, bg, bu, ad,
                  dg_o, du_o, gad_o, dx_o, qg_o, qu_o, acc, qg_acc, qu_acc, qd_s, qdt_s):
    step = pl.program_id(0)

    @pl.when(step == 0)
    def _():
        qd = keep(scale * mm(dy[...], bd[...], 1, 1), ids[...], rank)
        qd_s[...] = qd
        qdt_s[...] = qd.T
        acc[...] = jnp.zeros_like(acc)
        qg_acc[...] = jnp.zeros_like(qg_acc)
        qu_acc[...] = jnp.zeros_like(qu_acc)

    gate, up = gate_r[...], up_r[...]
    sig = jax.nn.sigmoid(gate)
    act = gate * sig
    gad_o[...] = mm(qdt_s[...], (act * up).astype(bf))
    dh = mm(dy[...], wd[...], 1, 1) + rounded(mm(qd_s[...], ad[...]))
    dg = (dh * up * sig * (1.0 + gate * (1.0 - sig))).astype(bf)
    du = (dh * act).astype(bf)
    dg_o[...] = dg
    du_o[...] = du
    acc[...] += mm(dg, wg[...], 1, 1) + mm(du, wu[...], 1, 1)
    qg_acc[...] += mm(dg, bg[...], 1, 1)
    qu_acc[...] += mm(du, bu[...], 1, 1)

    @pl.when(step == pl.num_programs(0) - 1)
    def _():
        qg = keep(scale * qg_acc[...], ids[...], rank)
        qu = keep(scale * qu_acc[...], ids[...], rank)
        qg_o[...] = qg
        qu_o[...] = qu
        lora = rounded(mm(qg, ag[...]) + mm(qu, au[...]))
        dx_o[...] = (dy[...].astype(f32) + acc[...] + lora).astype(bf)


def grads_body(scale, wide, pg, pu, pd, qg, qu, x, dy, dg, du, gbg, gbu, gag, gau, gbd, pgt, put, pdt, qgt, qut):
    step = pl.program_id(0)

    @pl.when(step == 0)
    def _():
        for src, dst in ((pg, pgt), (pu, put), (pd, pdt), (qg, qgt), (qu, qut)):
            dst[...] = src[...].T

    @pl.when(step < wide)
    def _():
        gbg[...] = scale * mm(pgt[...], dg[...])
        gbu[...] = scale * mm(put[...], du[...])

    @pl.when(step >= wide)
    def _():
        gag[...] = mm(qgt[...], x[...])
        gau[...] = mm(qut[...], x[...])
        gbd[...] = scale * mm(pdt[...], dy[...])


def whole(shape):
    return pl.BlockSpec(shape, lambda j: (0, 0), pipeline_mode=pl.Buffered(1))


def kept(shape):
    return pl.BlockSpec(shape, lambda j: (0, 0))


def cols(rows):
    return pl.BlockSpec((rows, TILE), lambda j: (0, j))


def params():
    return pltpu.CompilerParams(dimension_semantics=('arbitrary',), vmem_limit_bytes=60 * 2 ** 20)


def cost(flops, nbytes):
    return pl.CostEstimate(flops=flops, bytes_accessed=nbytes, transcendentals=0)


def solution(mesh):
    group = mesh.shape['data']
    tok_spec = P(('rep', 'data'), None)
    id_spec = P(('rep', 'data'))
    full_spec = P(None, None)
    own_spec = P('data', None, None)
    grad_spec = P(('rep', 'data'), None, None)

    def device_fn(x_loc, ids_loc, dy_loc, w_gate, w_up, w_down, a_gate, b_gate, a_up, b_up, a_down, b_down):
        tokens, dim = x_loc.shape
        n_local, _, rank = a_gate.shape
        hidden = w_gate.shape[1]
        width = n_local * rank
        scale = LORA_ALPHA / rank
        cap = ((3 * tokens + 8 * group - 1) // (8 * group)) * 8
        rows = group * cap
        steps = hidden // TILE
        owner = ids_loc // n_local
        local = ids_loc % n_local
        before = (owner[:, None] == owner[None, :]) & (jnp.arange(tokens)[None, :] < jnp.arange(tokens)[:, None])
        slot = owner * cap + before.astype(jnp.int32).sum(axis=1)
        hit = jnp.arange(rows)[:, None] == slot[None, :]
        pack = hit.astype(bf)
        slot_ids = jnp.where(hit, local[None, :] + 1, 0).max(axis=1) - 1

        def exchange(arr):
            return lax.all_to_all(arr, 'data', 0, 0, tiled=True)

        ids = exchange(slot_ids)[:, None]
        x = exchange(mm(pack, x_loc).astype(bf))
        dy = exchange(mm(pack, dy_loc).astype(bf))

        def as_rows(weight):
            return jnp.swapaxes(weight, 1, 2).reshape(width, weight.shape[1])

        ag, au, ad = as_rows(a_gate), as_rows(a_up), as_rows(a_down)
        bg, bu, bd = b_gate.reshape(width, hidden), b_up.reshape(width, hidden), b_down.reshape(width, dim)

        def arr(shape, dtype):
            return jax.ShapeDtypeStruct(shape, dtype)

        base = 2 * rows * dim * hidden
        lora = 2 * rows * width * hidden
        small = 2 * rows * width * dim
        shared = [whole((rows, 1)), whole((rows, dim)), whole((width, dim)), whole((width, dim)), whole((width, dim))]
        weights = [cols(dim), cols(dim), pl.BlockSpec((TILE, dim), lambda j: (j, 0)), cols(width), cols(width), cols(width)]
        gate, up, out, pg, pu, pd = pl.pallas_call(
            functools.partial(forward_body, rank, scale),
            grid=(steps,),
            in_specs=shared + weights,
            out_specs=[cols(rows), cols(rows), kept((rows, dim))] + [kept((rows, width))] * 3,
            out_shape=[arr((rows, hidden), f32)] * 2 + [arr((rows, dim), bf)] + [arr((rows, width), bf)] * 3,
            scratch_shapes=[pltpu.VMEM((rows, dim), f32), pltpu.VMEM((rows, width), f32)],
            compiler_params=params(),
            cost_estimate=cost(3 * base + 3 * lora + 3 * small, 6 * dim * hidden + 8 * rows * hidden),
            name='forward',
        )(ids, x, ag, au, bd, w_gate, w_up, w_down, bg, bu, ad)
        dg, du, g_ad, dx, qg, qu = pl.pallas_call(
            functools.partial(backward_body, rank, scale),
            grid=(steps,),
            in_specs=shared + [cols(rows), cols(rows)] + weights,
            out_specs=[cols(rows), cols(rows), cols(width), kept((rows, dim)), kept((rows, width)), kept((rows, width))],
            out_shape=[arr((rows, hidden), bf)] * 2 + [arr((width, hidden), f32), arr((rows, dim), bf)] + [arr((rows, width), bf)] * 2,
            scratch_shapes=[pltpu.VMEM((rows, dim), f32), pltpu.VMEM((rows, width), f32), pltpu.VMEM((rows, width), f32),
                            pltpu.VMEM((rows, width), bf), pltpu.VMEM((width, rows), bf)],
            compiler_params=params(),
            cost_estimate=cost(3 * base + 4 * lora + 3 * small, 6 * dim * hidden + 8 * rows * hidden),
            name='backward',
        )(ids, dy, ag, au, bd, gate, up, w_gate, w_up, w_down, bg, bu, ad)
        wide_cols = pl.BlockSpec((rows, TILE), lambda j: (0, jnp.minimum(j, steps - 1)))
        wide_grad = pl.BlockSpec((width, TILE), lambda j: (0, jnp.minimum(j, steps - 1)))
        slim_cols = pl.BlockSpec((rows, TILE), lambda j: (0, jnp.maximum(j - steps, 0)))
        slim_grad = pl.BlockSpec((width, TILE), lambda j: (0, jnp.maximum(j - steps, 0)))
        g_bg, g_bu, g_ag, g_au, g_bd = pl.pallas_call(
            functools.partial(grads_body, scale, steps),
            grid=(steps + dim // TILE,),
            in_specs=[whole((rows, width))] * 5 + [slim_cols, slim_cols, wide_cols, wide_cols],
            out_specs=[wide_grad, wide_grad, slim_grad, slim_grad, slim_grad],
            out_shape=[arr((width, hidden), f32)] * 2 + [arr((width, dim), f32)] * 3,
            scratch_shapes=[pltpu.VMEM((width, rows), bf)] * 5,
            compiler_params=params(),
            cost_estimate=cost(2 * lora + 3 * small, 8 * width * hidden),
            name='adapter_grads',
        )(pg, pu, pd, qg, qu, x, dy, dg, du)

        def back(vals):
            return mm(pack, exchange(vals), 0, 0).astype(bf)

        def a_grad(vals):
            return jnp.swapaxes(vals.reshape(n_local, rank, vals.shape[1]), 1, 2)

        def b_grad(vals):
            return vals.reshape(n_local, rank, vals.shape[1])

        return back(out), back(dx), a_grad(g_ag), b_grad(g_bg), a_grad(g_au), b_grad(g_bu), a_grad(g_ad), b_grad(g_bd)

    return jax.shard_map(
        device_fn,
        mesh=mesh,
        in_specs=(tok_spec, id_spec, tok_spec, full_spec, full_spec, full_spec) + (own_spec,) * 6,
        out_specs=(tok_spec, tok_spec) + (grad_spec,) * 6,
        check_vma=False,
    )
```

```python
import functools

import jax
import jax.numpy as jnp
from jax import lax
from jax.experimental import pallas as pl
from jax.experimental.pallas import tpu as pltpu
from jax.sharding import PartitionSpec as P

LORA_ALPHA = 32
TILE = 512
f32 = jnp.float32
bf = jnp.bfloat16


def mm(left, right, ldim=1, rdim=0):
    return lax.dot_general(left, right, (((ldim,), (rdim,)), ((), ())), preferred_element_type=f32)


def rounded(vals):
    return vals.astype(bf).astype(f32)


def keep(vals, ids, rank):
    cols = lax.div(lax.broadcasted_iota(jnp.int32, vals.shape, 1), jnp.int32(rank))
    return jnp.where(cols == ids, vals, 0.0).astype(bf)


def forward_body(cap, n_local, rank, scale, axes, ids_r, x_loc, dy_loc, ag_h, au_h, bd_h, wg, wu, wd, bg, bu, ad,
                 x_o, dy_o, gate_o, up_o, out_o, ids_o, pg_o, pu_o, pd_o,
                 gu, x_own, dy_own, xs, dys, ids_s, ids_v, wbuf, bbuf, small, acc, pd_acc,
                 send_sem, recv_sem, wsem, bsem, ssem, gsem, osem):
    group, dim = ids_s.shape[0], x_loc.shape[1]
    tokens, hidden = x_loc.shape[0], wg.shape[1]
    rows = group * cap
    part = wbuf.shape[1]
    n_slots = wbuf.shape[0]
    chunks = dim // part
    across = hidden // dim
    first = chunks * 2 * across
    steps = hidden // part
    rep, me = lax.axis_index(axes[0]), lax.axis_index(axes[1])

    def peer(k):
        return lax.rem(me + k, group)

    barrier = pltpu.get_barrier_semaphore()
    for k in range(1, group):
        pl.semaphore_signal(barrier, inc=1, device_id=(rep, peer(k)), device_id_type=pl.DeviceIdType.MESH)

    def tile_copy(src, slot):
        return pltpu.make_async_copy(src, wbuf.at[slot], wsem.at[slot])

    def start_tile(t):
        slot = lax.rem(t, n_slots)
        which = lax.rem(lax.div(t, across), 2)
        src = (pl.ds(pl.multiple_of(lax.div(t, 2 * across) * part, part), part),
               pl.ds(pl.multiple_of(lax.rem(t, across) * dim, dim), dim))

        @pl.when((t < first) & (which == 0))
        def _():
            tile_copy(wg.at[src], slot).start()

        @pl.when((t < first) & (which == 1))
        def _():
            tile_copy(wu.at[src], slot).start()

        @pl.when((t >= first) & (t < first + steps))
        def _():
            tile_copy(wd.at[pl.ds(pl.multiple_of((t - first) * part, part), part)], slot).start()

    def wait_tile(t):
        slot = lax.rem(t, n_slots)
        tile_copy(wd.at[pl.ds(0, part)], slot).wait()
        return slot

    def adapter_copies(j, slot):
        span = pl.ds(pl.multiple_of(j * part, part), part)
        return [pltpu.make_async_copy(src.at[:, span], bbuf.at[slot, i], bsem.at[slot, i]) for i, src in enumerate((bg, bu, ad))]

    small_copies = [pltpu.make_async_copy(src, small.at[i], ssem.at[i]) for i, src in enumerate((ag_h, au_h, bd_h))]

    def fill(t, carry):
        start_tile(t)
        return carry

    lax.fori_loop(0, n_slots, fill, 0)
    for copy in small_copies:
        copy.start()
    for j in range(2):
        for copy in adapter_copies(j, j):
            copy.start()

    ids = ids_r[...]
    owner = lax.div(ids, jnp.int32(n_local))
    local = lax.rem(ids, jnp.int32(n_local))
    owner_to = jnp.broadcast_to(owner.astype(f32), (tokens, tokens))
    earlier = lax.broadcasted_iota(jnp.int32, (tokens, tokens), 0) < lax.broadcasted_iota(jnp.int32, (tokens, tokens), 1)
    rank_in = jnp.sum(jnp.where((owner_to.T == owner_to) & earlier, 1.0, 0.0), axis=0, keepdims=True).astype(jnp.int32)
    pack = jnp.where(lax.broadcasted_iota(jnp.int32, (rows, tokens), 0) == owner * cap + rank_in, 1.0, 0.0).astype(bf)
    lanes = 128
    spread = jnp.where(lax.broadcasted_iota(jnp.int32, (group * lanes, tokens), 0) == owner * lanes + rank_in, 1.0, 0.0).astype(bf)
    tagged = mm(jnp.broadcast_to((local + 1).astype(f32), (8, tokens)).astype(bf), spread, 1, 1)
    for d in range(group):
        ids_s[d] = tagged[:, d * lanes:(d + 1) * lanes]

    def pack_part(src, dst, c):
        span = slice(c * part, (c + 1) * part)
        dst[:, span] = mm(pack, src[:, span]).astype(bf)

    mine = pl.ds(pl.multiple_of(me * cap, 16), cap)

    def row_copy(src, dst, span, c, k):
        there = pl.ds(pl.multiple_of(peer(k) * cap, 16), cap)
        return pltpu.make_async_remote_copy(
            src_ref=src.at[there, span], dst_ref=dst.at[mine, span], send_sem=send_sem.at[c, k], recv_sem=recv_sem.at[c, k],
            device_id=(rep, peer(k)), device_id_type=pl.DeviceIdType.MESH)

    def id_copy(k):
        return pltpu.make_async_remote_copy(
            src_ref=ids_s.at[peer(k)], dst_ref=ids_v.at[me], send_sem=send_sem.at[chunks + 1, k], recv_sem=recv_sem.at[chunks + 1, k],
            device_id=(rep, peer(k)), device_id_type=pl.DeviceIdType.MESH)

    x_copies = [[row_copy(xs, x_own, pl.ds(c * part, part), c, k) for k in range(1, group)] for c in range(chunks)]
    dy_copies = [row_copy(dys, dy_own, pl.ds(0, dim), chunks, k) for k in range(1, group)]
    id_copies = [id_copy(k) for k in range(1, group)]

    pack_part(x_loc, xs, 0)
    pl.semaphore_wait(barrier, group - 1)
    for c in range(chunks):
        if c + 1 < chunks:
            pack_part(x_loc, xs, c + 1)
        for copy in x_copies[c]:
            copy.start()
    for copy in id_copies:
        copy.start()
    for c in range(chunks):
        pack_part(dy_loc, dys, c)
    x_own[mine, :] = xs[mine, :]
    dy_own[mine, :] = dys[mine, :]
    ids_v[me] = ids_s[me]
    for copy in dy_copies:
        copy.start()

    def clear(i, carry):
        gu[0, pl.ds(pl.multiple_of(i * 8, 8), 8), :] = jnp.zeros((8, hidden), f32)
        gu[1, pl.ds(pl.multiple_of(i * 8, 8), 8), :] = jnp.zeros((8, hidden), f32)
        return carry

    lax.fori_loop(0, rows // 8, clear, 0)
    acc[...] = jnp.zeros_like(acc)
    pd_acc[...] = jnp.zeros_like(pd_acc)

    for c in range(chunks):
        for copy in x_copies[c]:
            copy.wait_recv()

        def pre_step(i, carry):
            t = c * 2 * across + i
            slot = wait_tile(t)
            span = pl.ds(pl.multiple_of(lax.rem(i, across) * dim, dim), dim)
            which = lax.div(i, across)
            gu[which, :, span] += mm(x_own[:, c * part:(c + 1) * part], wbuf[slot])
            start_tile(t + n_slots)
            return carry

        lax.fori_loop(0, 2 * across, pre_step, 0)

    for copy in id_copies:
        copy.wait_recv()
    got = jnp.concatenate([ids_v[s, 0:1, :] for s in range(group)] + [jnp.zeros((lanes - group, lanes), f32)], axis=0).T
    ids_col = jnp.concatenate([got[0:cap, s:s + 1] for s in range(group)], axis=0).astype(jnp.int32) - 1
    ids_o[...] = ids_col
    x_out = pltpu.make_async_copy(x_own, x_o, osem.at[0])
    x_out.start()
    for copy in small_copies[:2]:
        copy.wait()
    pg_o[...] = keep(mm(x_own[...], small[0], 1, 1), ids_col, rank)
    pu_o[...] = keep(mm(x_own[...], small[1], 1, 1), ids_col, rank)

    def gu_copies(j):
        span = pl.ds(pl.multiple_of(j * part, part), part)
        return [pltpu.make_async_copy(gu.at[i, :, span], dst.at[:, span], gsem.at[j, i]) for i, dst in enumerate((gate_o, up_o))]

    def step(j, carry):
        t = first + j
        span = pl.ds(pl.multiple_of(j * part, part), part)
        two = lax.rem(j, 2)
        for copy in adapter_copies(0, two):
            copy.wait()
        gate = gu[0, :, span] + rounded(scale * mm(pg_o[...], bbuf[two, 0]))
        up = gu[1, :, span] + rounded(scale * mm(pu_o[...], bbuf[two, 1]))
        gu[0, :, span] = gate
        gu[1, :, span] = up
        h = (gate * jax.nn.sigmoid(gate) * up).astype(bf)
        slot = wait_tile(t)
        acc[...] += mm(h, wbuf[slot])
        pd_acc[...] += mm(h, bbuf[two, 2], 1, 1)
        for copy in gu_copies(j):
            copy.start()
        start_tile(t + n_slots)

        @pl.when(j + 2 < steps)
        def _():
            for copy in adapter_copies(j + 2, two):
                copy.start()

        return carry

    lax.fori_loop(0, steps, step, 0)
    for copy in dy_copies:
        copy.wait_recv()
    dy_out = pltpu.make_async_copy(dy_own, dy_o, osem.at[1])
    dy_out.start()
    small_copies[2].wait()
    pd = keep(pd_acc[...], ids_col, rank)
    pd_o[...] = pd
    out_o[...] = (x_own[...].astype(f32) + acc[...] + rounded(scale * mm(pd, small[2]))).astype(bf)

    def drain(j, carry):
        for copy in gu_copies(j):
            copy.wait()
        return carry

    lax.fori_loop(0, steps, drain, 0)
    for copies in x_copies + [dy_copies, id_copies]:
        for copy in copies:
            copy.wait_send()
    x_out.wait()
    dy_out.wait()


def backward_body(rank, scale, ids, dy, ag, au, bd, gate_r, up_r, wg, wu, wd, bg, bu, ad,
                  dg_o, du_o, gad_o, dx_o, qg_o, qu_o, acc, qg_acc, qu_acc, qd_s, qdt_s):
    step = pl.program_id(0)

    @pl.when(step == 0)
    def _():
        qd = keep(scale * mm(dy[...], bd[...], 1, 1), ids[...], rank)
        qd_s[...] = qd
        qdt_s[...] = qd.T
        acc[...] = jnp.zeros_like(acc)
        qg_acc[...] = jnp.zeros_like(qg_acc)
        qu_acc[...] = jnp.zeros_like(qu_acc)

    gate, up = gate_r[...], up_r[...]
    sig = jax.nn.sigmoid(gate)
    act = gate * sig
    gad_o[...] = mm(qdt_s[...], (act * up).astype(bf))
    dh = mm(dy[...], wd[...], 1, 1) + rounded(mm(qd_s[...], ad[...]))
    dg = (dh * up * sig * (1.0 + gate * (1.0 - sig))).astype(bf)
    du = (dh * act).astype(bf)
    dg_o[...] = dg
    du_o[...] = du
    acc[...] += mm(dg, wg[...], 1, 1) + mm(du, wu[...], 1, 1)
    qg_acc[...] += mm(dg, bg[...], 1, 1)
    qu_acc[...] += mm(du, bu[...], 1, 1)

    @pl.when(step == pl.num_programs(0) - 1)
    def _():
        qg = keep(scale * qg_acc[...], ids[...], rank)
        qu = keep(scale * qu_acc[...], ids[...], rank)
        qg_o[...] = qg
        qu_o[...] = qu
        lora = rounded(mm(qg, ag[...]) + mm(qu, au[...]))
        dx_o[...] = (dy[...].astype(f32) + acc[...] + lora).astype(bf)


def grads_body(scale, wide, pg, pu, pd, qg, qu, x, dy, dg, du, gbg, gbu, gag, gau, gbd, pgt, put, pdt, qgt, qut):
    step = pl.program_id(0)

    @pl.when(step == 0)
    def _():
        for src, dst in ((pg, pgt), (pu, put), (pd, pdt), (qg, qgt), (qu, qut)):
            dst[...] = src[...].T

    @pl.when(step < wide)
    def _():
        gbg[...] = scale * mm(pgt[...], dg[...])
        gbu[...] = scale * mm(put[...], du[...])

    @pl.when(step >= wide)
    def _():
        gag[...] = mm(qgt[...], x[...])
        gau[...] = mm(qut[...], x[...])
        gbd[...] = scale * mm(pdt[...], dy[...])


def whole(shape):
    return pl.BlockSpec(shape, lambda j: (0, 0), pipeline_mode=pl.Buffered(1))


def kept(shape):
    return pl.BlockSpec(shape, lambda j: (0, 0))


def cols(rows):
    return pl.BlockSpec((rows, TILE), lambda j: (0, j))


def params():
    return pltpu.CompilerParams(dimension_semantics=('arbitrary',), vmem_limit_bytes=60 * 2 ** 20)


def cost(flops, nbytes):
    return pl.CostEstimate(flops=flops, bytes_accessed=nbytes, transcendentals=0)


def solution(mesh):
    group = mesh.shape['data']
    tok_spec = P(('rep', 'data'), None)
    id_spec = P(('rep', 'data'))
    full_spec = P(None, None)
    own_spec = P('data', None, None)
    grad_spec = P(('rep', 'data'), None, None)

    def device_fn(x_loc, ids_loc, dy_loc, w_gate, w_up, w_down, a_gate, b_gate, a_up, b_up, a_down, b_down):
        tokens, dim = x_loc.shape
        n_local, _, rank = a_gate.shape
        hidden = w_gate.shape[1]
        width = n_local * rank
        scale = LORA_ALPHA / rank
        cap = ((3 * tokens + 8 * group - 1) // (8 * group)) * 8
        rows = group * cap
        steps = hidden // TILE

        def exchange(arr):
            return lax.all_to_all(arr, 'data', 0, 0, tiled=True)

        def as_rows(weight):
            return jnp.swapaxes(weight, 1, 2).reshape(width, weight.shape[1])

        ag, au, ad = as_rows(a_gate), as_rows(a_up), as_rows(a_down)
        bg, bu, bd = b_gate.reshape(width, hidden), b_up.reshape(width, hidden), b_down.reshape(width, dim)

        def arr(shape, dtype):
            return jax.ShapeDtypeStruct(shape, dtype)

        base = 2 * rows * dim * hidden
        lora = 2 * rows * width * hidden
        small = 2 * rows * width * dim
        shared = [whole((rows, 1)), whole((rows, dim)), whole((width, dim)), whole((width, dim)), whole((width, dim))]
        weights = [cols(dim), cols(dim), pl.BlockSpec((TILE, dim), lambda j: (j, 0)), cols(width), cols(width), cols(width)]
        chunks = dim // TILE
        any_spec = pl.BlockSpec(memory_space=pl.ANY)
        vmem_spec = pl.BlockSpec(memory_space=pltpu.VMEM)
        sem = pltpu.SemaphoreType.DMA
        x, dy, gate, up, out, ids, pg, pu, pd = pl.pallas_call(
            functools.partial(forward_body, cap, n_local, rank, scale, mesh.axis_names),
            in_specs=[vmem_spec] * 3 + [any_spec] * 9,
            out_specs=[any_spec] * 4 + [vmem_spec] * 5,
            out_shape=[arr((rows, dim), bf)] * 2 + [arr((rows, hidden), f32)] * 2 + [arr((rows, dim), bf), arr((rows, 1), jnp.int32)]
            + [arr((rows, width), bf)] * 3,
            scratch_shapes=[
                pltpu.VMEM((2, rows, hidden), f32),
                pltpu.VMEM((rows, dim), bf), pltpu.VMEM((rows, dim), bf), pltpu.VMEM((rows, dim), bf), pltpu.VMEM((rows, dim), bf),
                pltpu.VMEM((group, 8, 128), f32), pltpu.VMEM((group, 8, 128), f32),
                pltpu.VMEM((4, TILE, dim), bf), pltpu.VMEM((2, 3, width, TILE), bf), pltpu.VMEM((3, width, dim), bf),
                pltpu.VMEM((rows, dim), f32), pltpu.VMEM((rows, width), f32),
                sem((chunks + 2, group)), sem((chunks + 2, group)), sem((4,)), sem((2, 3)), sem((3,)), sem((steps, 2)), sem((2,)),
            ],
            compiler_params=pltpu.CompilerParams(collective_id=0, has_side_effects=True, vmem_limit_bytes=63 * 2 ** 20),
            cost_estimate=cost(3 * base + 3 * lora + 3 * small, 6 * dim * hidden + 8 * rows * hidden),
            name='forward',
        )(ids_loc[None, :], x_loc, dy_loc, ag, au, bd, w_gate, w_up, w_down, bg, bu, ad)
        dg, du, g_ad, dx, qg, qu = pl.pallas_call(
            functools.partial(backward_body, rank, scale),
            grid=(steps,),
            in_specs=shared + [cols(rows), cols(rows)] + weights,
            out_specs=[cols(rows), cols(rows), cols(width), kept((rows, dim)), kept((rows, width)), kept((rows, width))],
            out_shape=[arr((rows, hidden), bf)] * 2 + [arr((width, hidden), f32), arr((rows, dim), bf)] + [arr((rows, width), bf)] * 2,
            scratch_shapes=[pltpu.VMEM((rows, dim), f32), pltpu.VMEM((rows, width), f32), pltpu.VMEM((rows, width), f32),
                            pltpu.VMEM((rows, width), bf), pltpu.VMEM((width, rows), bf)],
            compiler_params=params(),
            cost_estimate=cost(3 * base + 4 * lora + 3 * small, 6 * dim * hidden + 8 * rows * hidden),
            name='backward',
        )(ids, dy, ag, au, bd, gate, up, w_gate, w_up, w_down, bg, bu, ad)
        wide_cols = pl.BlockSpec((rows, TILE), lambda j: (0, jnp.minimum(j, steps - 1)))
        wide_grad = pl.BlockSpec((width, TILE), lambda j: (0, jnp.minimum(j, steps - 1)))
        slim_cols = pl.BlockSpec((rows, TILE), lambda j: (0, jnp.maximum(j - steps, 0)))
        slim_grad = pl.BlockSpec((width, TILE), lambda j: (0, jnp.maximum(j - steps, 0)))
        g_bg, g_bu, g_ag, g_au, g_bd = pl.pallas_call(
            functools.partial(grads_body, scale, steps),
            grid=(steps + dim // TILE,),
            in_specs=[whole((rows, width))] * 5 + [slim_cols, slim_cols, wide_cols, wide_cols],
            out_specs=[wide_grad, wide_grad, slim_grad, slim_grad, slim_grad],
            out_shape=[arr((width, hidden), f32)] * 2 + [arr((width, dim), f32)] * 3,
            scratch_shapes=[pltpu.VMEM((width, rows), bf)] * 5,
            compiler_params=params(),
            cost_estimate=cost(2 * lora + 3 * small, 8 * width * hidden),
            name='adapter_grads',
        )(pg, pu, pd, qg, qu, x, dy, dg, du)

        owner = ids_loc // n_local
        before = (owner[:, None] == owner[None, :]) & (jnp.arange(tokens)[None, :] < jnp.arange(tokens)[:, None])
        slot = owner * cap + before.astype(jnp.int32).sum(axis=1)
        pack = (jnp.arange(rows)[:, None] == slot[None, :]).astype(bf)

        def back(vals):
            return mm(pack, exchange(vals), 0, 0).astype(bf)

        def a_grad(vals):
            return jnp.swapaxes(vals.reshape(n_local, rank, vals.shape[1]), 1, 2)

        def b_grad(vals):
            return vals.reshape(n_local, rank, vals.shape[1])

        return back(out), back(dx), a_grad(g_ag), b_grad(g_bg), a_grad(g_au), b_grad(g_bu), a_grad(g_ad), b_grad(g_bd)

    return jax.shard_map(
        device_fn,
        mesh=mesh,
        in_specs=(tok_spec, id_spec, tok_spec, full_spec, full_spec, full_spec) + (own_spec,) * 6,
        out_specs=(tok_spec, tok_spec) + (grad_spec,) * 6,
        check_vma=False,
    )
```

```python
import functools

import jax
import jax.numpy as jnp
from jax import lax
from jax.experimental import pallas as pl
from jax.experimental.pallas import tpu as pltpu
from jax.sharding import PartitionSpec as P

LORA_ALPHA = 32
TILE = 512
WIDE = 1024
f32 = jnp.float32
bf = jnp.bfloat16


def mm(left, right, ldim=1, rdim=0):
    return lax.dot_general(left, right, (((ldim,), (rdim,)), ((), ())), preferred_element_type=f32)


def rounded(vals):
    return vals.astype(bf).astype(f32)


def keep(vals, ids, rank):
    cols = lax.div(lax.broadcasted_iota(jnp.int32, vals.shape, 1), jnp.int32(rank))
    return jnp.where(cols == ids, vals, 0.0).astype(bf)


def layer_body(cap, n_local, rank, scale, axes, ids_r, x_loc, dy_loc, ag_h, au_h, bd_h, wg, wu, wd, bg, bu, ad,
               x_o, dy_o, h_o, dg_o, du_o, dx_o, out_o, pack_o, pgt_o, put_o, qdt_o, pd_o, qg_o, qu_o,
               gu, x_own, dy_own, xs, dys, out_v, ids_s, ids_v, wbuf, bbuf, acc, qa, qb, pg, pu, qd, hbuf,
               send_sem, recv_sem, wsem, bsem, gsem, hsem, osem):
    group, dim = ids_s.shape[0], x_loc.shape[1]
    tokens, hidden = x_loc.shape[0], wg.shape[1]
    rows = group * cap
    n_slots, part = wbuf.shape[0], wbuf.shape[1]
    chunks = dim // part
    across = hidden // dim
    steps = hidden // part
    width = qa.shape[1]
    rep, me = lax.axis_index(axes[0]), lax.axis_index(axes[1])

    def peer(k):
        return lax.rem(me + k, group)

    barrier = pltpu.get_barrier_semaphore()
    for k in range(1, group):
        pl.semaphore_signal(barrier, inc=1, device_id=(rep, peer(k)), device_id_type=pl.DeviceIdType.MESH)

    def aligned(start, size, unit):
        return pl.ds(pl.multiple_of(start, unit), size)

    def start_tile(t, src):
        slot = lax.rem(t, n_slots)
        pltpu.make_async_copy(src, wbuf.at[slot], wsem.at[slot]).start()

    def wait_tile(t):
        slot = lax.rem(t, n_slots)
        pltpu.make_async_copy(bd_h, wbuf.at[slot], wsem.at[slot]).wait()
        return slot

    def block(ref, c, n):
        return ref.at[aligned(c * part, part, part), aligned(n * dim, dim, dim)]

    def start_pair(t, c, n):
        start_tile(t, block(wg, c, n))
        start_tile(t + 1, block(wu, c, n))

    def start_down(t, j):
        start_tile(t, wd.at[aligned(j * part, part, part)])

    def adapter_copies(j, slot):
        span = aligned(j * part, part, part)
        return [pltpu.make_async_copy(src.at[:, span], bbuf.at[slot, i], bsem.at[slot, i]) for i, src in enumerate((bg, bu, ad))]

    start_pair(0, 0, 0)
    start_pair(2, 0, 1)
    for j in range(2):
        for copy in adapter_copies(j, j):
            copy.start()

    ids = ids_r[...]
    owner = lax.div(ids, jnp.int32(n_local))
    local = lax.rem(ids, jnp.int32(n_local))
    owner_to = jnp.broadcast_to(owner.astype(f32), (tokens, tokens))
    earlier = lax.broadcasted_iota(jnp.int32, (tokens, tokens), 0) < lax.broadcasted_iota(jnp.int32, (tokens, tokens), 1)
    rank_in = jnp.sum(jnp.where((owner_to.T == owner_to) & earlier, 1.0, 0.0), axis=0, keepdims=True).astype(jnp.int32)
    pack = jnp.where(lax.broadcasted_iota(jnp.int32, (rows, tokens), 0) == owner * cap + rank_in, 1.0, 0.0).astype(bf)
    pack_o[...] = pack
    lanes = 128
    spread = jnp.where(lax.broadcasted_iota(jnp.int32, (group * lanes, tokens), 0) == owner * lanes + rank_in, 1.0, 0.0).astype(bf)
    tagged = mm(jnp.broadcast_to((local + 1).astype(f32), (8, tokens)).astype(bf), spread, 1, 1)
    for d in range(group):
        ids_s[d] = tagged[:, d * lanes:(d + 1) * lanes]

    def pack_part(src, dst, c):
        span = slice(c * part, (c + 1) * part)
        dst[:, span] = mm(pack, src[:, span]).astype(bf)

    mine = aligned(me * cap, cap, 16)

    def row_copy(src, dst, span, c, k):
        return pltpu.make_async_remote_copy(
            src_ref=src.at[aligned(peer(k) * cap, cap, 16), span], dst_ref=dst.at[mine, span],
            send_sem=send_sem.at[c, k], recv_sem=recv_sem.at[c, k],
            device_id=(rep, peer(k)), device_id_type=pl.DeviceIdType.MESH)

    def id_copy(k):
        return pltpu.make_async_remote_copy(
            src_ref=ids_s.at[peer(k)], dst_ref=ids_v.at[me], send_sem=send_sem.at[chunks + 1, k], recv_sem=recv_sem.at[chunks + 1, k],
            device_id=(rep, peer(k)), device_id_type=pl.DeviceIdType.MESH)

    others = range(1, group)
    x_copies = [[row_copy(xs, x_own, pl.ds(c * part, part), c, k) for k in others] for c in range(chunks)]
    dy_copies = [row_copy(dys, dy_own, pl.ds(0, dim), chunks, k) for k in others]
    id_copies = [id_copy(k) for k in others]
    out_copies = [row_copy(xs, out_v, pl.ds(0, dim), chunks + 2, k) for k in others]

    pack_part(x_loc, xs, 0)
    pl.semaphore_wait(barrier, group - 1)
    for c in range(chunks):
        if c + 1 < chunks:
            pack_part(x_loc, xs, c + 1)
        for copy in x_copies[c]:
            copy.start()
    for copy in id_copies:
        copy.start()
    for c in range(chunks):
        pack_part(dy_loc, dys, c)
    x_own[mine, :] = xs[mine, :]
    dy_own[mine, :] = dys[mine, :]
    ids_v[me] = ids_s[me]
    for copy in dy_copies:
        copy.start()

    def clear(i, carry):
        gu[0, aligned(i * 8, 8, 8), :] = jnp.zeros((8, hidden), f32)
        gu[1, aligned(i * 8, 8, 8), :] = jnp.zeros((8, hidden), f32)
        return carry

    lax.fori_loop(0, rows // 8, clear, 0)
    acc[...] = jnp.zeros_like(acc)
    qa[...] = jnp.zeros_like(qa)
    qb[...] = jnp.zeros_like(qb)

    pairs = chunks * across
    for c in range(chunks):
        for copy in x_copies[c]:
            copy.wait_recv()

        def pre_step(n, carry):
            p = c * across + n
            ahead = p + 2

            @pl.when(ahead < pairs)
            def _():
                start_pair(2 * ahead, lax.div(ahead, across), lax.rem(ahead, across))

            if c == chunks - 1:
                @pl.when(ahead == pairs)
                def _():
                    start_tile(2 * pairs, ag_h)
                    start_tile(2 * pairs + 1, au_h)

                @pl.when(ahead == pairs + 1)
                def _():
                    start_down(2 * pairs + 2, 0)
                    start_down(2 * pairs + 3, 1)

            span = aligned(n * dim, dim, dim)
            one, two = wait_tile(2 * p), wait_tile(2 * p + 1)
            gu[0, :, span] += mm(x_own[:, c * part:(c + 1) * part], wbuf[one])
            gu[1, :, span] += mm(x_own[:, c * part:(c + 1) * part], wbuf[two])
            return carry

        lax.fori_loop(0, across, pre_step, 0)

    base = 2 * pairs
    start_down(base + 4, 2)
    start_down(base + 5, 3)
    for copy in id_copies:
        copy.wait_recv()
    got = jnp.concatenate([ids_v[s, 0:1, :] for s in range(group)] + [jnp.zeros((lanes - group, lanes), f32)], axis=0).T
    ids_col = jnp.concatenate([got[0:cap, s:s + 1] for s in range(group)], axis=0).astype(jnp.int32) - 1
    x_out = pltpu.make_async_copy(x_own, x_o, osem.at[0])
    x_out.start()
    one, two = wait_tile(base), wait_tile(base + 1)
    pg[...] = keep(mm(x_own[...], wbuf[one], 1, 1), ids_col, rank)
    pu[...] = keep(mm(x_own[...], wbuf[two], 1, 1), ids_col, rank)
    base += 2

    def h_copy(j, two):
        return pltpu.make_async_copy(hbuf.at[two], h_o.at[:, aligned(j * part, part, part)], hsem.at[two])

    def step(j, carry):
        t = base + j

        @pl.when(j + 4 < steps)
        def _():
            start_down(t + 4, j + 4)

        @pl.when(j + 4 == steps)
        def _():
            start_tile(t + 4, bd_h)

        @pl.when(j + 4 > steps)
        def _():
            start_down(t + 4, j + 3 - steps)

        span = aligned(j * part, part, part)
        two = lax.rem(j, 2)

        @pl.when(j >= 2)
        def _():
            h_copy(0, two).wait()

        for copy in adapter_copies(0, two):
            copy.wait()
        slot = wait_tile(t)
        gate = gu[0, :, span] + rounded(scale * mm(pg[...], bbuf[two, 0]))
        up = gu[1, :, span] + rounded(scale * mm(pu[...], bbuf[two, 1]))
        gu[0, :, span] = gate
        gu[1, :, span] = up
        h = (gate * jax.nn.sigmoid(gate) * up).astype(bf)
        hbuf[two] = h
        slab = aligned(lax.rem(j, width // lanes) * lanes, lanes, lanes)
        pgt_o[slab, :] = pg[:, slab].T
        put_o[slab, :] = pu[:, slab].T
        acc[...] += mm(h, wbuf[slot])
        qa[...] += mm(h, bbuf[two, 2], 1, 1)
        h_copy(j, two).start()
        for copy in adapter_copies(lax.rem(j + 2, steps), two):
            copy.start()
        return carry

    lax.fori_loop(0, steps, step, 0)
    for two in range(2):
        h_copy(0, two).wait()
    base += steps
    start_down(base + 4, 3)
    for copy in dy_copies:
        copy.wait_recv()
    dy_out = pltpu.make_async_copy(dy_own, dy_o, osem.at[1])
    dy_out.start()
    for copies in x_copies:
        for copy in copies:
            copy.wait_send()
    slot = wait_tile(base)
    pd = keep(qa[...], ids_col, rank)
    pd_o[...] = pd
    xs[...] = (x_own[...].astype(f32) + acc[...] + rounded(scale * mm(pd, wbuf[slot]))).astype(bf)
    qd[...] = keep(scale * mm(dy_own[...], wbuf[slot], 1, 1), ids_col, rank)
    for copy in out_copies:
        copy.start()
    out_v[mine, :] = xs[mine, :]
    acc[...] = jnp.zeros_like(acc)
    qa[...] = jnp.zeros_like(qa)
    base += 1
    x_out.wait()
    for copy in dy_copies:
        copy.wait_send()

    per = dim // part
    width_tiles = 3 * per

    def grad_copies(j, i):
        span = aligned(j * part, part, part)
        here = aligned(i * part, part, part)
        return [pltpu.make_async_copy(src.at[:, here], dst.at[:, span], gsem.at[i, n])
                for n, (src, dst) in enumerate(((x_own, dg_o), (dys, du_o)))]

    def super_step(s, carry):
        first = base + s * width_tiles

        def sub_step(k, carry):
            start_pair(first + per + 2 * k, k, s)
            for ii in range(2):
                i = 2 * k + ii
                j = s * per + i
                span = aligned(j * part, part, part)
                here = aligned(i * part, part, part)

                @pl.when(s > 0)
                def _():
                    for copy in grad_copies(0, i):
                        copy.wait()

                for copy in adapter_copies(0, ii):
                    copy.wait()
                slot = wait_tile(first + i)
                gate, up = gu[0, :, span], gu[1, :, span]
                sig = jax.nn.sigmoid(gate)
                act = gate * sig
                dh = mm(dy_own[...], wbuf[slot], 1, 1) + rounded(mm(qd[...], bbuf[ii, 2]))
                dg = (dh * up * sig * (1.0 + gate * (1.0 - sig))).astype(bf)
                du = (dh * act).astype(bf)
                x_own[:, here] = dg
                dys[:, here] = du
                slab = aligned(lax.rem(j, width // lanes) * lanes, lanes, lanes)
                qdt_o[slab, :] = qd[:, slab].T
                qa[...] += mm(dg, bbuf[ii, 0], 1, 1)
                qb[...] += mm(du, bbuf[ii, 1], 1, 1)
                for copy in grad_copies(j, i):
                    copy.start()

                @pl.when(j + 2 < steps)
                def _():
                    for copy in adapter_copies(j + 2, ii):
                        copy.start()

            return carry

        lax.fori_loop(0, per // 2, sub_step, 0)

        def dx_step(d, carry):
            t = first + per + 2 * d

            @pl.when(d < per - 2)
            def _():
                start_pair(t + 4, d + 2, s)

            @pl.when((d >= per - 2) & (s < across - 1))
            def _():
                j = (s + 1) * per + 2 * (d - (per - 2))
                start_down(t + 4, j)
                start_down(t + 5, j + 1)

            @pl.when((d == per - 2) & (s == across - 1))
            def _():
                start_tile(t + 4, ag_h)
                start_tile(t + 5, au_h)

            here = aligned(d * part, part, part)
            one, two = wait_tile(t), wait_tile(t + 1)
            acc[:, here] += mm(x_own[...], wbuf[one], 1, 1) + mm(dys[...], wbuf[two], 1, 1)
            return carry

        lax.fori_loop(0, per, dx_step, 0)
        return carry

    lax.fori_loop(0, across, super_step, 0)
    base += across * width_tiles
    one, two = wait_tile(base), wait_tile(base + 1)
    qg = keep(scale * qa[...], ids_col, rank)
    qu = keep(scale * qb[...], ids_col, rank)
    qg_o[...] = qg
    qu_o[...] = qu
    lora = rounded(mm(qg, wbuf[one]) + mm(qu, wbuf[two]))
    for i in range(per):
        for copy in grad_copies(0, i):
            copy.wait()
    dys[...] = (dy_own[...].astype(f32) + acc[...] + lora).astype(bf)
    dx_out = pltpu.make_async_copy(dys, dx_o, osem.at[2])
    dx_out.start()
    for copy in out_copies:
        copy.wait_recv()
    out_o[...] = mm(pack_o[...], out_v[...], 0, 0).astype(bf)
    for copies in (id_copies, out_copies):
        for copy in copies:
            copy.wait_send()
    dy_out.wait()
    dx_out.wait()


def grads_body(scale, wide, pgt, put, qdt, pd, qg, qu, x, dy, h, dg, du, gbg, gbu, gad, gag, gau, gbd, pdt, qgt, qut):
    step = pl.program_id(0)

    @pl.when(step == wide)
    def _():
        for src, dst in ((pd, pdt), (qg, qgt), (qu, qut)):
            dst[...] = src[...].T

    @pl.when(step < wide)
    def _():
        gbg[...] = scale * mm(pgt[...], dg[...])
        gbu[...] = scale * mm(put[...], du[...])
        gad[...] = mm(qdt[...], h[...])

    @pl.when(step >= wide)
    def _():
        gag[...] = mm(qgt[...], x[...])
        gau[...] = mm(qut[...], x[...])
        gbd[...] = scale * mm(pdt[...], dy[...])


def whole(shape):
    return pl.BlockSpec(shape, lambda j: (0, 0), pipeline_mode=pl.Buffered(1))


def params():
    return pltpu.CompilerParams(dimension_semantics=('arbitrary',), vmem_limit_bytes=60 * 2 ** 20)


def cost(flops, nbytes):
    return pl.CostEstimate(flops=flops, bytes_accessed=nbytes, transcendentals=0)


def solution(mesh):
    group = mesh.shape['data']
    tok_spec = P(('rep', 'data'), None)
    id_spec = P(('rep', 'data'))
    full_spec = P(None, None)
    own_spec = P('data', None, None)
    grad_spec = P(('rep', 'data'), None, None)

    def device_fn(x_loc, ids_loc, dy_loc, w_gate, w_up, w_down, a_gate, b_gate, a_up, b_up, a_down, b_down):
        tokens, dim = x_loc.shape
        n_local, _, rank = a_gate.shape
        hidden = w_gate.shape[1]
        width = n_local * rank
        scale = LORA_ALPHA / rank
        cap = ((3 * tokens + 8 * group - 1) // (8 * group)) * 8
        rows = group * cap
        steps = hidden // TILE

        def exchange(arr):
            return lax.all_to_all(arr, 'data', 0, 0, tiled=True)

        def as_rows(weight):
            return jnp.swapaxes(weight, 1, 2).reshape(width, weight.shape[1])

        ag, au, ad = as_rows(a_gate), as_rows(a_up), as_rows(a_down)
        bg, bu, bd = b_gate.reshape(width, hidden), b_up.reshape(width, hidden), b_down.reshape(width, dim)

        def arr(shape, dtype):
            return jax.ShapeDtypeStruct(shape, dtype)

        base = 2 * rows * dim * hidden
        lora = 2 * rows * width * hidden
        small = 2 * rows * width * dim
        chunks = dim // TILE
        any_spec = pl.BlockSpec(memory_space=pl.ANY)
        vmem_spec = pl.BlockSpec(memory_space=pltpu.VMEM)
        sem = pltpu.SemaphoreType.DMA
        x, dy, h, dg, du, dx, out, pack, pgt, put, qdt, pd, qg, qu = pl.pallas_call(
            functools.partial(layer_body, cap, n_local, rank, scale, mesh.axis_names),
            in_specs=[vmem_spec] * 3 + [any_spec] * 9,
            out_specs=[any_spec] * 6 + [vmem_spec] * 8,
            out_shape=[arr((rows, dim), bf)] * 2 + [arr((rows, hidden), bf)] * 3 + [arr((rows, dim), bf), arr((tokens, dim), bf), arr((rows, tokens), bf)]
            + [arr((width, rows), bf)] * 3 + [arr((rows, width), bf)] * 3,
            scratch_shapes=[
                pltpu.VMEM((2, rows, hidden), f32),
                pltpu.VMEM((rows, dim), bf), pltpu.VMEM((rows, dim), bf), pltpu.VMEM((rows, dim), bf), pltpu.VMEM((rows, dim), bf),
                pltpu.VMEM((rows, dim), bf),
                pltpu.VMEM((group, 8, 128), f32), pltpu.VMEM((group, 8, 128), f32),
                pltpu.VMEM((6, TILE, dim), bf), pltpu.VMEM((2, 3, width, TILE), bf),
                pltpu.VMEM((rows, dim), f32), pltpu.VMEM((rows, width), f32), pltpu.VMEM((rows, width), f32),
                pltpu.VMEM((rows, width), bf), pltpu.VMEM((rows, width), bf), pltpu.VMEM((rows, width), bf), pltpu.VMEM((2, rows, TILE), bf),
                sem((chunks + 3, group)), sem((chunks + 3, group)), sem((6,)), sem((2, 3)), sem((dim // TILE, 2)), sem((2,)), sem((3,)),
            ],
            compiler_params=pltpu.CompilerParams(collective_id=0, has_side_effects=True, vmem_limit_bytes=67043328),
            cost_estimate=cost(6 * base + 6 * lora + 6 * small, 12 * dim * hidden),
            name='layer',
        )(ids_loc[None, :], x_loc, dy_loc, ag, au, bd, w_gate, w_up, w_down, bg, bu, ad)
        steps = hidden // WIDE
        wide_cols = pl.BlockSpec((rows, WIDE), lambda j: (0, jnp.minimum(j, steps - 1)))
        wide_grad = pl.BlockSpec((width, WIDE), lambda j: (0, jnp.minimum(j, steps - 1)))
        slim_cols = pl.BlockSpec((rows, TILE), lambda j: (0, jnp.maximum(j - steps, 0)))
        slim_grad = pl.BlockSpec((width, TILE), lambda j: (0, jnp.maximum(j - steps, 0)))
        g_bg, g_bu, g_ad, g_ag, g_au, g_bd = pl.pallas_call(
            functools.partial(grads_body, scale, steps),
            grid=(steps + dim // TILE,),
            in_specs=[whole((width, rows))] * 3 + [whole((rows, width))] * 3 + [slim_cols, slim_cols, wide_cols, wide_cols, wide_cols],
            out_specs=[wide_grad, wide_grad, wide_grad, slim_grad, slim_grad, slim_grad],
            out_shape=[arr((width, hidden), f32)] * 3 + [arr((width, dim), f32)] * 3,
            scratch_shapes=[pltpu.VMEM((width, rows), bf)] * 3,
            compiler_params=params(),
            cost_estimate=cost(3 * lora + 3 * small, 12 * width * hidden),
            name='adapter_grads',
        )(pgt, put, qdt, pd, qg, qu, x, dy, h, dg, du)

        def back(vals):
            return mm(pack, exchange(vals), 0, 0).astype(bf)

        def a_grad(vals):
            return jnp.swapaxes(vals.reshape(n_local, rank, vals.shape[1]), 1, 2)

        def b_grad(vals):
            return vals.reshape(n_local, rank, vals.shape[1])

        return out, back(dx), a_grad(g_ag), b_grad(g_bg), a_grad(g_au), b_grad(g_bu), a_grad(g_ad), b_grad(g_bd)

    return jax.shard_map(
        device_fn,
        mesh=mesh,
        in_specs=(tok_spec, id_spec, tok_spec, full_spec, full_spec, full_spec) + (own_spec,) * 6,
        out_specs=(tok_spec, tok_spec) + (grad_spec,) * 6,
        check_vma=False,
    )
```

```python
import functools

import jax
import jax.numpy as jnp
from jax import lax
from jax.experimental import pallas as pl
from jax.experimental.pallas import tpu as pltpu
from jax.sharding import PartitionSpec as P

LORA_ALPHA = 32
TILE = 512
DEEP = 4
f32 = jnp.float32
bf = jnp.bfloat16


def mm(left, right, ldim=1, rdim=0):
    return lax.dot_general(left, right, (((ldim,), (rdim,)), ((), ())), preferred_element_type=f32)


def rounded(vals):
    return vals.astype(bf).astype(f32)


def keep(vals, ids, rank):
    cols = lax.div(lax.broadcasted_iota(jnp.int32, vals.shape, 1), jnp.int32(rank))
    return jnp.where(cols == ids, vals, 0.0).astype(bf)


def layer_body(cap, n_local, rank, scale, axes, ids_r, x_loc, dy_loc, ag_h, au_h, bd_h, wg, wu, wd, bg, bu, ad,
               x_o, dy_o, h_o, dg_o, du_o, dx_o, out_o, pack_o, pgt_o, put_o, qdt_o, pd_o, qg_o, qu_o,
               gu, x_own, dy_own, xs, dys, out_v, ids_s, ids_v, wbuf, bbuf, acc, qa, qb, pg, pu, qd,
               send_sem, recv_sem, wsem, bsem, gsem, hsem, osem):
    group, dim = ids_s.shape[0], x_loc.shape[1]
    tokens, hidden = x_loc.shape[0], wg.shape[1]
    rows = group * cap
    n_slots, part = wbuf.shape[0], wbuf.shape[1]
    chunks = dim // part
    across = hidden // dim
    steps = hidden // part
    width = qa.shape[1]
    rep, me = lax.axis_index(axes[0]), lax.axis_index(axes[1])

    def peer(k):
        return lax.rem(me + k, group)

    barrier = pltpu.get_barrier_semaphore()
    for k in range(1, group):
        pl.semaphore_signal(barrier, inc=1, device_id=(rep, peer(k)), device_id_type=pl.DeviceIdType.MESH)

    def aligned(start, size, unit):
        return pl.ds(pl.multiple_of(start, unit), size)

    def start_tile(t, src):
        slot = lax.rem(t, n_slots)
        pltpu.make_async_copy(src, wbuf.at[slot], wsem.at[slot]).start()

    def wait_tile(t):
        slot = lax.rem(t, n_slots)
        pltpu.make_async_copy(bd_h, wbuf.at[slot], wsem.at[slot]).wait()
        return slot

    def block(ref, c, n):
        return ref.at[aligned(c * part, part, part), aligned(n * dim, dim, dim)]

    def start_pair(t, c, n):
        start_tile(t, block(wg, c, n))
        start_tile(t + 1, block(wu, c, n))

    def start_down(t, j):
        start_tile(t, wd.at[aligned(j * part, part, part)])

    def adapter_copies(j, slot):
        span = aligned(j * part, part, part)
        return [pltpu.make_async_copy(src.at[:, span], bbuf.at[slot, i], bsem.at[slot, i]) for i, src in enumerate((bg, bu, ad))]

    def adapter_copy(j, slot, i):
        span = aligned(j * part, part, part)
        return pltpu.make_async_copy((bg, bu, ad)[i].at[:, span], bbuf.at[slot, i], bsem.at[slot, i])

    def refill(j, which):
        for ii in range(2):
            for i in which:
                adapter_copy(lax.rem(j + 2 + ii, steps), ii, i).start()

    def wait_adapters(which):
        for ii in range(2):
            for i in which:
                adapter_copy(0, ii, i).wait()

    start_pair(0, 0, 0)
    start_pair(2, 0, 1)
    for j in range(2):
        for i in range(3):
            adapter_copy(j, j, i).start()

    ids = ids_r[...]
    owner = lax.div(ids, jnp.int32(n_local))
    local = lax.rem(ids, jnp.int32(n_local))
    owner_to = jnp.broadcast_to(owner.astype(f32), (tokens, tokens))
    earlier = lax.broadcasted_iota(jnp.int32, (tokens, tokens), 0) < lax.broadcasted_iota(jnp.int32, (tokens, tokens), 1)
    rank_in = jnp.sum(jnp.where((owner_to.T == owner_to) & earlier, 1.0, 0.0), axis=0, keepdims=True).astype(jnp.int32)
    pack = jnp.where(lax.broadcasted_iota(jnp.int32, (rows, tokens), 0) == owner * cap + rank_in, 1.0, 0.0).astype(bf)
    pack_o[...] = pack
    lanes = 128
    spread = jnp.where(lax.broadcasted_iota(jnp.int32, (group * lanes, tokens), 0) == owner * lanes + rank_in, 1.0, 0.0).astype(bf)
    tagged = mm(jnp.broadcast_to((local + 1).astype(f32), (8, tokens)).astype(bf), spread, 1, 1)
    for d in range(group):
        ids_s[d] = tagged[:, d * lanes:(d + 1) * lanes]

    def pack_part(src, dst, c):
        span = slice(c * part, (c + 1) * part)
        dst[:, span] = mm(pack, src[:, span]).astype(bf)

    mine = aligned(me * cap, cap, 16)

    def row_copy(src, dst, span, c, k):
        return pltpu.make_async_remote_copy(
            src_ref=src.at[aligned(peer(k) * cap, cap, 16), span], dst_ref=dst.at[mine, span],
            send_sem=send_sem.at[c, k], recv_sem=recv_sem.at[c, k],
            device_id=(rep, peer(k)), device_id_type=pl.DeviceIdType.MESH)

    def id_copy(k):
        return pltpu.make_async_remote_copy(
            src_ref=ids_s.at[peer(k)], dst_ref=ids_v.at[me], send_sem=send_sem.at[chunks + 1, k], recv_sem=recv_sem.at[chunks + 1, k],
            device_id=(rep, peer(k)), device_id_type=pl.DeviceIdType.MESH)

    others = range(1, group)
    x_copies = [[row_copy(xs, x_own, pl.ds(c * part, part), c, k) for k in others] for c in range(chunks)]
    dy_copies = [row_copy(dys, dy_own, pl.ds(0, dim), chunks, k) for k in others]
    id_copies = [id_copy(k) for k in others]
    out_copies = [row_copy(xs, out_v, pl.ds(0, dim), chunks + 2, k) for k in others]

    pack_part(x_loc, xs, 0)
    pl.semaphore_wait(barrier, group - 1)
    for c in range(chunks):
        if c + 1 < chunks:
            pack_part(x_loc, xs, c + 1)
        for copy in x_copies[c]:
            copy.start()
    for copy in id_copies:
        copy.start()
    for c in range(chunks):
        pack_part(dy_loc, dys, c)
    x_own[mine, :] = xs[mine, :]
    dy_own[mine, :] = dys[mine, :]
    ids_v[me] = ids_s[me]
    for copy in dy_copies:
        copy.start()

    def clear(i, carry):
        gu[0, aligned(i * 8, 8, 8), :] = jnp.zeros((8, hidden), f32)
        gu[1, aligned(i * 8, 8, 8), :] = jnp.zeros((8, hidden), f32)
        return carry

    lax.fori_loop(0, rows // 8, clear, 0)
    acc[...] = jnp.zeros_like(acc)
    qa[...] = jnp.zeros_like(qa)
    qb[...] = jnp.zeros_like(qb)

    pairs = chunks * across
    for c in range(chunks):
        for copy in x_copies[c]:
            copy.wait_recv()

        last = c == chunks - 1

        def ahead(p):
            start_pair(2 * p, lax.div(p, across), lax.rem(p, across))

        def pre_step(i, carry, last_step=False):
            p = c * across + 2 * i
            if last_step:
                start_tile(2 * pairs, ag_h)
                start_tile(2 * pairs + 1, au_h)
            else:
                ahead(p + 2)
            for half in range(2):
                t = 2 * (p + half)
                span = aligned((2 * i + half) * dim, dim, dim)
                one, two = wait_tile(t), wait_tile(t + 1)
                gu[0, :, span] += mm(x_own[:, c * part:(c + 1) * part], wbuf[one])
                gu[1, :, span] += mm(x_own[:, c * part:(c + 1) * part], wbuf[two])
                if half == 0 and last_step:
                    start_down(2 * pairs + 2, 0)
                    start_down(2 * pairs + 3, 1)
                elif half == 0:
                    ahead(p + 3)
            return carry

        turns = across // 2
        lax.fori_loop(0, turns - 1 if last else turns, pre_step, 0)
        if last:
            pre_step(turns - 1, 0, True)

    base = 2 * pairs
    start_down(base + 4, 2)
    start_down(base + 5, 3)
    for copy in id_copies:
        copy.wait_recv()
    got = jnp.concatenate([ids_v[s, 0:1, :] for s in range(group)] + [jnp.zeros((lanes - group, lanes), f32)], axis=0).T
    ids_col = jnp.concatenate([got[0:cap, s:s + 1] for s in range(group)], axis=0).astype(jnp.int32) - 1
    x_out = pltpu.make_async_copy(x_own, x_o, osem.at[0])
    x_out.start()
    one, two = wait_tile(base), wait_tile(base + 1)
    pg[...] = keep(mm(x_own[...], wbuf[one], 1, 1), ids_col, rank)
    pu[...] = keep(mm(x_own[...], wbuf[two], 1, 1), ids_col, rank)
    base += 2

    def h_copy(j, two):
        return pltpu.make_async_copy(dys.at[:, pl.ds(two * part, part)], h_o.at[:, aligned(j * part, part, part)], hsem.at[two])

    for copy in dy_copies:
        copy.wait_send()

    def step(jj, carry):
        j = 2 * jj
        t = base + j

        @pl.when(j + 4 < steps)
        def _():
            start_down(t + 4, j + 4)
            start_down(t + 5, j + 5)

        @pl.when(j + 4 == steps)
        def _():
            start_tile(t + 4, bd_h)
            start_down(t + 5, 0)

        @pl.when(j + 4 > steps)
        def _():
            start_down(t + 4, 1)
            start_down(t + 5, 2)

        @pl.when(jj > 0)
        def _():
            for ii in range(2):
                h_copy(0, ii).wait()

        wait_adapters((0, 1))
        slots = [wait_tile(t), wait_tile(t + 1)]
        for ii in range(2):
            span = aligned((j + ii) * part, part, part)
            gate = gu[0, :, span] + rounded(scale * mm(pg[...], bbuf[ii, 0]))
            up = gu[1, :, span] + rounded(scale * mm(pu[...], bbuf[ii, 1]))
            gu[0, :, span] = gate
            gu[1, :, span] = up
            dys[:, ii * part:(ii + 1) * part] = (gate * jax.nn.sigmoid(gate) * up).astype(bf)
        refill(j, (0, 1))
        for ii in range(2):
            h_copy(j + ii, ii).start()
        slab = aligned(lax.rem(jj, width // lanes) * lanes, lanes, lanes)
        pgt_o[slab, :] = pg[:, slab].T
        put_o[slab, :] = pu[:, slab].T
        wait_adapters((2,))
        for ii in range(2):
            h = dys[:, ii * part:(ii + 1) * part]
            acc[...] += mm(h, wbuf[slots[ii]])
            qa[...] += mm(h, bbuf[ii, 2], 1, 1)
        refill(j, (2,))
        return carry

    lax.fori_loop(0, steps // 2, step, 0)
    for two in range(2):
        h_copy(0, two).wait()
    base += steps
    start_down(base + 4, 3)
    for copy in dy_copies:
        copy.wait_recv()
    dy_out = pltpu.make_async_copy(dy_own, dy_o, osem.at[1])
    dy_out.start()
    for copies in x_copies:
        for copy in copies:
            copy.wait_send()
    slot = wait_tile(base)
    pd = keep(qa[...], ids_col, rank)
    pd_o[...] = pd
    xs[...] = (x_own[...].astype(f32) + acc[...] + rounded(scale * mm(pd, wbuf[slot]))).astype(bf)
    qd[...] = keep(scale * mm(dy_own[...], wbuf[slot], 1, 1), ids_col, rank)
    for copy in out_copies:
        copy.start()
    out_v[mine, :] = xs[mine, :]
    acc[...] = jnp.zeros_like(acc)
    qa[...] = jnp.zeros_like(qa)
    base += 1
    x_out.wait()

    per = dim // part
    width_tiles = 3 * per

    def grad_copies(j, i):
        span = aligned(j * part, part, part)
        here = aligned(i * part, part, part)
        return [pltpu.make_async_copy(src.at[:, here], dst.at[:, span], gsem.at[i, n])
                for n, (src, dst) in enumerate(((x_own, dg_o), (dys, du_o)))]

    def super_step(s, carry):
        first = base + s * width_tiles

        def sub_step(k, carry):
            i0 = 2 * k
            j0 = s * per + i0
            start_pair(first + per + i0, k, s)

            @pl.when(s > 0)
            def _():
                for ii in range(2):
                    for copy in grad_copies(0, i0 + ii):
                        copy.wait()

            wait_adapters((2,))
            slots = [wait_tile(first + i0), wait_tile(first + i0 + 1)]
            for ii in range(2):
                span = aligned((j0 + ii) * part, part, part)
                here = aligned((i0 + ii) * part, part, part)
                gate, up = gu[0, :, span], gu[1, :, span]
                sig = jax.nn.sigmoid(gate)
                act = gate * sig
                dh = mm(dy_own[...], wbuf[slots[ii]], 1, 1) + rounded(mm(qd[...], bbuf[ii, 2]))
                x_own[:, here] = (dh * up * sig * (1.0 + gate * (1.0 - sig))).astype(bf)
                dys[:, here] = (dh * act).astype(bf)
            refill(j0, (2,))
            slab = aligned(lax.rem(lax.div(j0, 2), width // lanes) * lanes, lanes, lanes)
            qdt_o[slab, :] = qd[:, slab].T
            wait_adapters((0, 1))
            for ii in range(2):
                here = aligned((i0 + ii) * part, part, part)
                qa[...] += mm(x_own[:, here], bbuf[ii, 0], 1, 1)
                qb[...] += mm(dys[:, here], bbuf[ii, 1], 1, 1)
                for copy in grad_copies(j0 + ii, i0 + ii):
                    copy.start()
            refill(j0, (0, 1))
            return carry

        lax.fori_loop(0, per // 2, sub_step, 0)

        for turn in range(per // 2):
            final = turn == per // 2 - 1
            t0 = first + per + 4 * turn
            nxt = jnp.minimum((s + 1) * per, steps - per)
            if final:
                @pl.when(s < across - 1)
                def _():
                    start_down(t0 + 4, nxt)
                    start_down(t0 + 5, nxt + 1)

                @pl.when(s == across - 1)
                def _():
                    start_tile(t0 + 4, ag_h)
                    start_tile(t0 + 5, au_h)
            else:
                start_pair(t0 + 4, 2 * turn + 2, s)
            for half in range(2):
                d = 2 * turn + half
                t = t0 + 2 * half
                here = slice(d * part, (d + 1) * part)
                one, two = wait_tile(t), wait_tile(t + 1)
                acc[:, here] += mm(x_own[...], wbuf[one], 1, 1) + mm(dys[...], wbuf[two], 1, 1)
                if half == 0 and final:
                    start_down(t0 + 6, nxt + 2)
                    start_down(t0 + 7, nxt + 3)
                elif half == 0:
                    start_pair(t0 + 6, 2 * turn + 3, s)
        return carry

    lax.fori_loop(0, across, super_step, 0)
    base += across * width_tiles
    one, two = wait_tile(base), wait_tile(base + 1)
    wait_tile(base + 2)
    wait_tile(base + 3)
    wait_adapters((0, 1, 2))
    qg = keep(scale * qa[...], ids_col, rank)
    qu = keep(scale * qb[...], ids_col, rank)
    qg_o[...] = qg
    qu_o[...] = qu
    lora = rounded(mm(qg, wbuf[one]) + mm(qu, wbuf[two]))
    for i in range(per):
        for copy in grad_copies(0, i):
            copy.wait()
    dys[...] = (dy_own[...].astype(f32) + acc[...] + lora).astype(bf)
    dx_out = pltpu.make_async_copy(dys, dx_o, osem.at[2])
    dx_out.start()
    for copy in out_copies:
        copy.wait_recv()
    out_o[...] = mm(pack_o[...], out_v[...], 0, 0).astype(bf)
    for copies in (id_copies, out_copies):
        for copy in copies:
            copy.wait_send()
    dy_out.wait()
    dx_out.wait()


def grads_body(scale, pgt_h, put_h, qdt_h, pd_h, qg_h, qu_h, x_h, dy_h, h, dg, du, gbg, gbu, gad, gag, gau, gbd,
               lefts, flat, turned, rows_v, ins, outs, lsem, fsem, rsem, isem, xsem):
    deep, part = ins.shape[0], ins.shape[3]
    wide, slim = dg.shape[1] // part, x_h.shape[1] // part
    sources, targets, tails = (dg, du, h), (gbg, gbu, gad), (gag, gau, gbd)

    def span(j):
        return pl.ds(pl.multiple_of(j * part, part), part)

    def in_copy(j, i):
        slot = lax.rem(j, deep)
        return pltpu.make_async_copy(sources[i].at[:, span(j)], ins.at[slot, i], isem.at[slot, i])

    def out_copy(dst, j, n, i):
        slot = lax.rem(n, deep)
        return pltpu.make_async_copy(outs.at[slot, i], dst.at[:, span(j)], xsem.at[slot, i])

    left_copies = [pltpu.make_async_copy(src, lefts.at[i], lsem.at[i]) for i, src in enumerate((pgt_h, put_h, qdt_h))]
    flat_copies = [pltpu.make_async_copy(src, flat.at[i], fsem.at[i]) for i, src in enumerate((qg_h, qu_h, pd_h))]
    row_copies = [pltpu.make_async_copy(src, rows_v.at[i], rsem.at[i]) for i, src in enumerate((x_h, dy_h))]
    for i in range(3):
        left_copies[i].start()
        in_copy(0, i).start()
    for j in range(1, deep):
        for i in range(3):
            in_copy(j, i).start()
    for copy in flat_copies + row_copies:
        copy.start()
    for copy in left_copies:
        copy.wait()

    def wide_step(j, carry):
        slot = lax.rem(j, deep)
        for i in range(3):
            in_copy(j, i).wait()

            @pl.when(j >= deep)
            def _():
                out_copy(targets[i], 0, j, i).wait()

            vals = mm(lefts[i], ins[slot, i])
            outs[slot, i] = vals if i == 2 else scale * vals
            out_copy(targets[i], j, j, i).start()

        @pl.when(j + deep < wide)
        def _():
            for i in range(3):
                in_copy(j + deep, i).start()

        return carry

    lax.fori_loop(0, wide, wide_step, 0)
    for i in range(3):
        flat_copies[i].wait()
        turned[i] = flat[i].T
    for copy in row_copies:
        copy.wait()

    def slim_step(j, carry):
        n = wide + j
        slot = lax.rem(n, deep)
        for i in range(3):
            out_copy(tails[i], 0, n, i).wait()
            vals = mm(turned[i], rows_v[i // 2, :, span(j)])
            outs[slot, i] = scale * vals if i == 2 else vals
            out_copy(tails[i], j, n, i).start()
        return carry

    lax.fori_loop(0, slim, slim_step, 0)
    for n in range(deep):
        for i in range(3):
            out_copy(tails[i], 0, n, i).wait()


def cost(flops, nbytes):
    return pl.CostEstimate(flops=flops, bytes_accessed=nbytes, transcendentals=0)


def solution(mesh):
    group = mesh.shape['data']
    tok_spec = P(('rep', 'data'), None)
    id_spec = P(('rep', 'data'))
    full_spec = P(None, None)
    own_spec = P('data', None, None)
    grad_spec = P(('rep', 'data'), None, None)

    def device_fn(x_loc, ids_loc, dy_loc, w_gate, w_up, w_down, a_gate, b_gate, a_up, b_up, a_down, b_down):
        tokens, dim = x_loc.shape
        n_local, _, rank = a_gate.shape
        hidden = w_gate.shape[1]
        width = n_local * rank
        scale = LORA_ALPHA / rank
        cap = ((3 * tokens + 8 * group - 1) // (8 * group)) * 8
        rows = group * cap
        steps = hidden // TILE

        def exchange(arr):
            return lax.all_to_all(arr, 'data', 0, 0, tiled=True)

        def as_rows(weight):
            return jnp.swapaxes(weight, 1, 2).reshape(width, weight.shape[1])

        ag, au, ad = as_rows(a_gate), as_rows(a_up), as_rows(a_down)
        bg, bu, bd = b_gate.reshape(width, hidden), b_up.reshape(width, hidden), b_down.reshape(width, dim)

        def arr(shape, dtype):
            return jax.ShapeDtypeStruct(shape, dtype)

        base = 2 * rows * dim * hidden
        lora = 2 * rows * width * hidden
        small = 2 * rows * width * dim
        chunks = dim // TILE
        any_spec = pl.BlockSpec(memory_space=pl.ANY)
        vmem_spec = pl.BlockSpec(memory_space=pltpu.VMEM)
        sem = pltpu.SemaphoreType.DMA
        x, dy, h, dg, du, dx, out, pack, pgt, put, qdt, pd, qg, qu = pl.pallas_call(
            functools.partial(layer_body, cap, n_local, rank, scale, mesh.axis_names),
            in_specs=[vmem_spec] * 3 + [any_spec] * 9,
            out_specs=[any_spec] * 6 + [vmem_spec] * 8,
            out_shape=[arr((rows, dim), bf)] * 2 + [arr((rows, hidden), bf)] * 3 + [arr((rows, dim), bf), arr((tokens, dim), bf), arr((rows, tokens), bf)]
            + [arr((width, rows), bf)] * 3 + [arr((rows, width), bf)] * 3,
            scratch_shapes=[
                pltpu.VMEM((2, rows, hidden), f32),
                pltpu.VMEM((rows, dim), bf), pltpu.VMEM((rows, dim), bf), pltpu.VMEM((rows, dim), bf), pltpu.VMEM((rows, dim), bf),
                pltpu.VMEM((rows, dim), bf),
                pltpu.VMEM((group, 8, 128), f32), pltpu.VMEM((group, 8, 128), f32),
                pltpu.VMEM((6, TILE, dim), bf), pltpu.VMEM((2, 3, width, TILE), bf),
                pltpu.VMEM((rows, dim), f32), pltpu.VMEM((rows, width), f32), pltpu.VMEM((rows, width), f32),
                pltpu.VMEM((rows, width), bf), pltpu.VMEM((rows, width), bf), pltpu.VMEM((rows, width), bf),
                sem((chunks + 3, group)), sem((chunks + 3, group)), sem((6,)), sem((2, 3)), sem((dim // TILE, 2)), sem((2,)), sem((3,)),
            ],
            compiler_params=pltpu.CompilerParams(collective_id=0, has_side_effects=True, vmem_limit_bytes=67043328),
            cost_estimate=cost(6 * base + 6 * lora + 6 * small, 12 * dim * hidden),
            name='layer',
        )(ids_loc[None, :], x_loc, dy_loc, ag, au, bd, w_gate, w_up, w_down, bg, bu, ad)
        g_bg, g_bu, g_ad, g_ag, g_au, g_bd = pl.pallas_call(
            functools.partial(grads_body, scale),
            in_specs=[any_spec] * 11,
            out_specs=[any_spec] * 6,
            out_shape=[arr((width, hidden), f32)] * 3 + [arr((width, dim), f32)] * 3,
            scratch_shapes=[
                pltpu.VMEM((3, width, rows), bf), pltpu.VMEM((3, rows, width), bf), pltpu.VMEM((3, width, rows), bf), pltpu.VMEM((2, rows, dim), bf),
                pltpu.VMEM((DEEP, 3, rows, TILE), bf), pltpu.VMEM((DEEP, 3, width, TILE), f32),
                sem((3,)), sem((3,)), sem((2,)), sem((DEEP, 3)), sem((DEEP, 3)),
            ],
            compiler_params=pltpu.CompilerParams(vmem_limit_bytes=60 * 2 ** 20),
            cost_estimate=cost(3 * lora + 3 * small, 12 * width * hidden),
            name='adapter_grads',
        )(pgt, put, qdt, pd, qg, qu, x, dy, h, dg, du)

        def back(vals):
            return mm(pack, exchange(vals), 0, 0).astype(bf)

        def a_grad(vals):
            return jnp.swapaxes(vals.reshape(n_local, rank, vals.shape[1]), 1, 2)

        def b_grad(vals):
            return vals.reshape(n_local, rank, vals.shape[1])

        return out, back(dx), a_grad(g_ag), b_grad(g_bg), a_grad(g_au), b_grad(g_bu), a_grad(g_ad), b_grad(g_bd)

    return jax.shard_map(
        device_fn,
        mesh=mesh,
        in_specs=(tok_spec, id_spec, tok_spec, full_spec, full_spec, full_spec) + (own_spec,) * 6,
        out_specs=(tok_spec, tok_spec) + (grad_spec,) * 6,
        check_vma=False,
    )
```

```python
import functools

import jax
import jax.numpy as jnp
from jax import lax
from jax.experimental import pallas as pl
from jax.experimental.pallas import tpu as pltpu
from jax.sharding import PartitionSpec as P

LORA_ALPHA = 32
TILE = 512
DEEP = 6
f32 = jnp.float32
bf = jnp.bfloat16


def mm(left, right, ldim=1, rdim=0):
    return lax.dot_general(left, right, (((ldim,), (rdim,)), ((), ())), preferred_element_type=f32)


def rounded(vals):
    return vals.astype(bf).astype(f32)


def keep(vals, ids, rank):
    cols = lax.div(lax.broadcasted_iota(jnp.int32, vals.shape, 1), jnp.int32(rank))
    return jnp.where(cols == ids, vals, 0.0).astype(bf)


def layer_body(cap, n_local, rank, scale, axes, ids_r, x_in, dy_in, ag_h, au_h, bd_h, wg, wu, wd, bg, bu, ad,
               x_o, dy_o, h_o, dg_o, du_o, dx_o, out_o, pack_o, pgt_o, put_o, qdt_o, pd_o, qg_o, qu_o,
               gu, x_own, dy_own, xs, dys, out_v, ids_s, ids_v, wbuf, bbuf, acc, qa, qb, pg, pu,
               send_sem, recv_sem, wsem, bsem, gsem, hsem, osem):
    group, dim = ids_s.shape[0], x_in.shape[1]
    tokens, hidden = x_in.shape[0], wg.shape[1]
    rows = group * cap
    n_slots, part = wbuf.shape[0], wbuf.shape[1]
    chunks = dim // part
    across = hidden // dim
    steps = hidden // part
    width = qa.shape[1]
    rep, me = lax.axis_index(axes[0]), lax.axis_index(axes[1])

    def peer(k):
        return lax.rem(me + k, group)

    barrier = pltpu.get_barrier_semaphore()
    for k in range(1, group):
        pl.semaphore_signal(barrier, inc=1, device_id=(rep, peer(k)), device_id_type=pl.DeviceIdType.MESH)

    def aligned(start, size, unit):
        return pl.ds(pl.multiple_of(start, unit), size)

    def start_tile(t, src):
        slot = lax.rem(t, n_slots)
        pltpu.make_async_copy(src, wbuf.at[slot], wsem.at[slot]).start()

    def wait_tile(t):
        slot = lax.rem(t, n_slots)
        pltpu.make_async_copy(bd_h, wbuf.at[slot], wsem.at[slot]).wait()
        return slot

    def block(ref, c, n):
        return ref.at[aligned(c * part, part, part), aligned(n * dim, dim, dim)]

    def start_pair(t, c, n):
        start_tile(t, block(wg, c, n))
        start_tile(t + 1, block(wu, c, n))

    def start_down(t, j):
        start_tile(t, wd.at[aligned(j * part, part, part)])

    def adapter_copies(j, slot):
        span = aligned(j * part, part, part)
        return [pltpu.make_async_copy(src.at[:, span], bbuf.at[slot, i], bsem.at[slot, i]) for i, src in enumerate((bg, bu, ad))]

    def adapter_copy(j, slot, i):
        span = aligned(j * part, part, part)
        return pltpu.make_async_copy((bg, bu, ad)[i].at[:, span], bbuf.at[slot, i], bsem.at[slot, i])

    def refill(j, which):
        for ii in range(2):
            for i in which:
                adapter_copy(lax.rem(j + 2 + ii, steps), ii, i).start()

    def wait_adapters(which):
        for ii in range(2):
            for i in which:
                adapter_copy(0, ii, i).wait()

    x_loc, dy_loc = out_v.at[pl.ds(0, tokens)], out_v.at[pl.ds(tokens, tokens)]
    in_copies = [pltpu.make_async_copy(src, dst, osem.at[i]) for i, (src, dst) in enumerate(((x_in, x_loc), (dy_in, dy_loc)))]
    for copy in in_copies:
        copy.start()
    start_pair(0, 0, 0)
    start_pair(2, 0, 1)
    for j in range(2):
        for i in range(3):
            adapter_copy(j, j, i).start()

    ids = ids_r[...]
    owner = lax.div(ids, jnp.int32(n_local))
    local = lax.rem(ids, jnp.int32(n_local))
    owner_to = jnp.broadcast_to(owner.astype(f32), (tokens, tokens))
    earlier = lax.broadcasted_iota(jnp.int32, (tokens, tokens), 0) < lax.broadcasted_iota(jnp.int32, (tokens, tokens), 1)
    rank_in = jnp.sum(jnp.where((owner_to.T == owner_to) & earlier, 1.0, 0.0), axis=0, keepdims=True).astype(jnp.int32)
    pack = jnp.where(lax.broadcasted_iota(jnp.int32, (rows, tokens), 0) == owner * cap + rank_in, 1.0, 0.0).astype(bf)
    pack_o[...] = pack
    lanes = 128

    def pack_part(src, dst, c):
        span = slice(c * part, (c + 1) * part)
        dst[:, span] = mm(pack, src[:, span]).astype(bf)

    mine = aligned(me * cap, cap, 16)

    def row_copy(src, dst, span, c, k):
        return pltpu.make_async_remote_copy(
            src_ref=src.at[aligned(peer(k) * cap, cap, 16), span], dst_ref=dst.at[mine, span],
            send_sem=send_sem.at[c, k], recv_sem=recv_sem.at[c, k],
            device_id=(rep, peer(k)), device_id_type=pl.DeviceIdType.MESH)

    def id_copy(k):
        return pltpu.make_async_remote_copy(
            src_ref=ids_s.at[peer(k)], dst_ref=ids_v.at[me], send_sem=send_sem.at[chunks + 1, k], recv_sem=recv_sem.at[chunks + 1, k],
            device_id=(rep, peer(k)), device_id_type=pl.DeviceIdType.MESH)

    others = range(1, group)
    x_copies = [[row_copy(xs, x_own, pl.ds(c * part, part), c, k) for k in others] for c in range(chunks)]
    dy_copies = [row_copy(dys, dy_own, pl.ds(0, dim), chunks, k) for k in others]
    id_copies = [id_copy(k) for k in others]
    out_copies = [row_copy(xs, out_v, pl.ds(0, dim), chunks + 2, k) for k in others]

    in_copies[0].wait()
    pack_part(x_loc, xs, 0)
    pl.semaphore_wait(barrier, group - 1)
    for c in range(chunks):
        if c + 1 < chunks:
            pack_part(x_loc, xs, c + 1)
        for copy in x_copies[c]:
            copy.start()
    spread = jnp.where(lax.broadcasted_iota(jnp.int32, (group * lanes, tokens), 0) == owner * lanes + rank_in, 1.0, 0.0).astype(bf)
    tagged = mm(jnp.broadcast_to((local + 1).astype(f32), (8, tokens)).astype(bf), spread, 1, 1)
    for d in range(group):
        ids_s[d] = tagged[:, d * lanes:(d + 1) * lanes]
    for copy in id_copies:
        copy.start()
    in_copies[1].wait()
    for c in range(chunks):
        pack_part(dy_loc, dys, c)
    x_own[mine, :] = xs[mine, :]
    dy_own[mine, :] = dys[mine, :]
    ids_v[me] = ids_s[me]
    for copy in dy_copies:
        copy.start()

    def clear(i, carry):
        gu[0, aligned(i * 8, 8, 8), :] = jnp.zeros((8, hidden), f32)
        gu[1, aligned(i * 8, 8, 8), :] = jnp.zeros((8, hidden), f32)
        return carry

    lax.fori_loop(0, rows // 8, clear, 0)
    acc[...] = jnp.zeros_like(acc)
    qa[...] = jnp.zeros_like(qa)
    qb[...] = jnp.zeros_like(qb)

    pairs = chunks * across
    for c in range(chunks):
        for copy in x_copies[c]:
            copy.wait_recv()

        last = c == chunks - 1

        def ahead(p):
            start_pair(2 * p, lax.div(p, across), lax.rem(p, across))

        def pre_step(i, carry, last_step=False):
            p = c * across + 2 * i
            t = 2 * p
            if last_step:
                start_tile(2 * pairs, ag_h)
                start_tile(2 * pairs + 1, au_h)
                start_down(2 * pairs + 2, 0)
                start_down(2 * pairs + 3, 1)
            else:
                ahead(p + 2)
                ahead(p + 3)
            slots = [wait_tile(t + n) for n in range(4)]
            for half in range(2):
                span = aligned((2 * i + half) * dim, dim, dim)
                gu[0, :, span] += mm(x_own[:, c * part:(c + 1) * part], wbuf[slots[2 * half]])
                gu[1, :, span] += mm(x_own[:, c * part:(c + 1) * part], wbuf[slots[2 * half + 1]])
            return carry

        turns = across // 2
        lax.fori_loop(0, turns - 1 if last else turns, pre_step, 0)
        if last:
            pre_step(turns - 1, 0, True)

    base = 2 * pairs
    start_down(base + 4, 2)
    start_down(base + 5, 3)
    for copy in id_copies:
        copy.wait_recv()
    got = jnp.concatenate([ids_v[s, 0:1, :] for s in range(group)] + [jnp.zeros((lanes - group, lanes), f32)], axis=0).T
    ids_col = jnp.concatenate([got[0:cap, s:s + 1] for s in range(group)], axis=0).astype(jnp.int32) - 1
    x_out = pltpu.make_async_copy(x_own, x_o, osem.at[0])
    x_out.start()
    one, two = wait_tile(base), wait_tile(base + 1)
    pg[...] = keep(mm(x_own[...], wbuf[one], 1, 1), ids_col, rank)
    pu[...] = keep(mm(x_own[...], wbuf[two], 1, 1), ids_col, rank)
    base += 2

    def h_copy(j, two):
        return pltpu.make_async_copy(dys.at[:, pl.ds(two * part, part)], h_o.at[:, aligned(j * part, part, part)], hsem.at[two])

    for copy in dy_copies:
        copy.wait_send()

    def step(jj, carry):
        j = 2 * jj
        t = base + j

        @pl.when(j + 4 < steps)
        def _():
            start_down(t + 4, j + 4)
            start_down(t + 5, j + 5)

        @pl.when(j + 4 == steps)
        def _():
            start_tile(t + 4, bd_h)
            start_down(t + 5, 0)

        @pl.when(j + 4 > steps)
        def _():
            start_down(t + 4, 1)
            start_down(t + 5, 2)

        @pl.when(jj > 0)
        def _():
            for ii in range(2):
                h_copy(0, ii).wait()

        wait_adapters((0, 1))
        slots = [wait_tile(t), wait_tile(t + 1)]
        for ii in range(2):
            span = aligned((j + ii) * part, part, part)
            gate = gu[0, :, span] + rounded(scale * mm(pg[...], bbuf[ii, 0]))
            up = gu[1, :, span] + rounded(scale * mm(pu[...], bbuf[ii, 1]))
            gu[0, :, span] = gate
            gu[1, :, span] = up
            dys[:, ii * part:(ii + 1) * part] = (gate * jax.nn.sigmoid(gate) * up).astype(bf)
        refill(j, (0, 1))
        for ii in range(2):
            h_copy(j + ii, ii).start()
        slab = aligned(lax.rem(jj, width // lanes) * lanes, lanes, lanes)
        pgt_o[slab, :] = pg[:, slab].T
        put_o[slab, :] = pu[:, slab].T
        wait_adapters((2,))
        for ii in range(2):
            h = dys[:, ii * part:(ii + 1) * part]
            acc[...] += mm(h, wbuf[slots[ii]])
            qa[...] += mm(h, bbuf[ii, 2], 1, 1)
        refill(j, (2,))
        return carry

    lax.fori_loop(0, steps // 2, step, 0)
    for two in range(2):
        h_copy(0, two).wait()
    base += steps
    start_down(base + 4, 3)
    for copy in dy_copies:
        copy.wait_recv()
    dy_out = pltpu.make_async_copy(dy_own, dy_o, osem.at[1])
    dy_out.start()
    for copies in x_copies:
        for copy in copies:
            copy.wait_send()
    slot = wait_tile(base)
    pd = keep(qa[...], ids_col, rank)
    pg[...] = pd
    pd_out = pltpu.make_async_copy(pg, pd_o, osem.at[3])
    pd_out.start()
    xs[...] = (x_own[...].astype(f32) + acc[...] + rounded(scale * mm(pd, wbuf[slot]))).astype(bf)
    pu[...] = keep(scale * mm(dy_own[...], wbuf[slot], 1, 1), ids_col, rank)
    for copy in out_copies:
        copy.start()
    out_v[mine, :] = xs[mine, :]
    acc[...] = jnp.zeros_like(acc)
    qa[...] = jnp.zeros_like(qa)
    base += 1
    x_out.wait()

    per = dim // part
    width_tiles = 3 * per

    def grad_copies(j, i):
        span = aligned(j * part, part, part)
        here = aligned(i * part, part, part)
        return [pltpu.make_async_copy(src.at[:, here], dst.at[:, span], gsem.at[i, n])
                for n, (src, dst) in enumerate(((x_own, dg_o), (dys, du_o)))]

    def super_step(s, carry):
        first = base + s * width_tiles

        def sub_step(k, carry):
            i0 = 2 * k
            j0 = s * per + i0
            start_pair(first + per + i0, k, s)

            @pl.when(s > 0)
            def _():
                for ii in range(2):
                    for copy in grad_copies(0, i0 + ii):
                        copy.wait()

            wait_adapters((2,))
            slots = [wait_tile(first + i0), wait_tile(first + i0 + 1)]
            for ii in range(2):
                span = aligned((j0 + ii) * part, part, part)
                here = aligned((i0 + ii) * part, part, part)
                gate, up = gu[0, :, span], gu[1, :, span]
                sig = jax.nn.sigmoid(gate)
                act = gate * sig
                dh = mm(dy_own[...], wbuf[slots[ii]], 1, 1) + rounded(mm(pu[...], bbuf[ii, 2]))
                x_own[:, here] = (dh * up * sig * (1.0 + gate * (1.0 - sig))).astype(bf)
                dys[:, here] = (dh * act).astype(bf)
            refill(j0, (2,))
            slab = aligned(lax.rem(lax.div(j0, 2), width // lanes) * lanes, lanes, lanes)
            qdt_o[slab, :] = pu[:, slab].T
            wait_adapters((0, 1))
            for ii in range(2):
                here = aligned((i0 + ii) * part, part, part)
                qa[...] += mm(x_own[:, here], bbuf[ii, 0], 1, 1)
                qb[...] += mm(dys[:, here], bbuf[ii, 1], 1, 1)
                for copy in grad_copies(j0 + ii, i0 + ii):
                    copy.start()
            refill(j0, (0, 1))
            return carry

        lax.fori_loop(0, per // 2, sub_step, 0)

        for turn in range(per // 2):
            t0 = first + per + 4 * turn
            if turn == per // 2 - 1:
                @pl.when(s < across - 1)
                def _():
                    for n in range(4):
                        start_down(t0 + 4 + n, (s + 1) * per + n)

                @pl.when(s == across - 1)
                def _():
                    start_tile(t0 + 4, ag_h)
                    start_tile(t0 + 5, au_h)
            else:
                start_pair(t0 + 4, 2 * turn + 2, s)
                start_pair(t0 + 6, 2 * turn + 3, s)
            slots = [wait_tile(t0 + n) for n in range(4)]
            for half in range(2):
                d = 2 * turn + half
                here = slice(d * part, (d + 1) * part)
                acc[:, here] += mm(x_own[...], wbuf[slots[2 * half]], 1, 1) + mm(dys[...], wbuf[slots[2 * half + 1]], 1, 1)
        return carry

    lax.fori_loop(0, across, super_step, 0)
    base += across * width_tiles
    one, two = wait_tile(base), wait_tile(base + 1)
    wait_adapters((0, 1, 2))
    qg = keep(scale * qa[...], ids_col, rank)
    qu = keep(scale * qb[...], ids_col, rank)
    pd_out.wait()
    pg[...] = qg
    pu[...] = qu
    q_outs = [pltpu.make_async_copy(src, dst, osem.at[3 + i]) for i, (src, dst) in enumerate(((pg, qg_o), (pu, qu_o)))]
    for copy in q_outs:
        copy.start()
    lora = rounded(mm(qg, wbuf[one]) + mm(qu, wbuf[two]))
    for i in range(per):
        for copy in grad_copies(0, i):
            copy.wait()
    dys[...] = (dy_own[...].astype(f32) + acc[...] + lora).astype(bf)
    dx_out = pltpu.make_async_copy(dys, dx_o, osem.at[2])
    dx_out.start()
    for copy in out_copies:
        copy.wait_recv()
    out_o[...] = mm(pack_o[...], out_v[...], 0, 0).astype(bf)
    for copies in (id_copies, out_copies):
        for copy in copies:
            copy.wait_send()
    dy_out.wait()
    dx_out.wait()
    for copy in q_outs:
        copy.wait()


def grads_body(scale, pgt_h, put_h, qdt_h, pd_h, qg_h, qu_h, x_h, dy_h, h, dg, du, gbg, gbu, gad, gag, gau, gbd,
               lefts, flat, turned, rows_v, ins, outs, lsem, fsem, rsem, isem, xsem):
    deep, part = ins.shape[0], ins.shape[3]
    wide, slim = dg.shape[1] // part, x_h.shape[1] // part
    sources, targets, tails = (dg, du, h), (gbg, gbu, gad), (gag, gau, gbd)

    def span(j):
        return pl.ds(pl.multiple_of(j * part, part), part)

    def in_copy(j, i):
        slot = lax.rem(j, deep)
        return pltpu.make_async_copy(sources[i].at[:, span(j)], ins.at[slot, i], isem.at[slot, i])

    def out_copy(dst, j, n, i):
        slot = lax.rem(n, deep)
        return pltpu.make_async_copy(outs.at[slot, i], dst.at[:, span(j)], xsem.at[slot, i])

    left_copies = [pltpu.make_async_copy(src, lefts.at[i], lsem.at[i]) for i, src in enumerate((pgt_h, put_h, qdt_h))]
    flat_copies = [pltpu.make_async_copy(src, flat.at[i], fsem.at[i]) for i, src in enumerate((qg_h, qu_h, pd_h))]
    row_copies = [pltpu.make_async_copy(src, rows_v.at[i], rsem.at[i]) for i, src in enumerate((x_h, dy_h))]
    for i in range(3):
        left_copies[i].start()
        in_copy(0, i).start()
    for j in range(1, deep):
        for i in range(3):
            in_copy(j, i).start()
    for copy in flat_copies + row_copies:
        copy.start()
    for copy in left_copies:
        copy.wait()

    def wide_step(jj, carry):
        j = 2 * jj
        for n in range(2):
            for i in range(3):
                in_copy(j + n, i).wait()

        @pl.when(j >= deep)
        def _():
            for n in range(2):
                for i in range(3):
                    out_copy(targets[i], 0, j + n, i).wait()

        for n in range(2):
            slot = lax.rem(j + n, deep)
            for i in range(3):
                vals = mm(lefts[i], ins[slot, i])
                outs[slot, i] = vals if i == 2 else scale * vals
                out_copy(targets[i], j + n, j + n, i).start()

        @pl.when(j + deep < wide)
        def _():
            for n in range(2):
                for i in range(3):
                    in_copy(j + n + deep, i).start()

        return carry

    lax.fori_loop(0, wide // 2, wide_step, 0)
    for i in range(3):
        flat_copies[i].wait()
        turned[i] = flat[i].T
    for copy in row_copies:
        copy.wait()

    def slim_step(j, carry):
        n = wide + j
        slot = lax.rem(n, deep)
        for i in range(3):
            out_copy(tails[i], 0, n, i).wait()
            vals = mm(turned[i], rows_v[i // 2, :, span(j)])
            outs[slot, i] = scale * vals if i == 2 else vals
            out_copy(tails[i], j, n, i).start()
        return carry

    lax.fori_loop(0, slim, slim_step, 0)
    for n in range(deep):
        for i in range(3):
            out_copy(tails[i], 0, n, i).wait()


def cost(flops, nbytes):
    return pl.CostEstimate(flops=flops, bytes_accessed=nbytes, transcendentals=0)


def solution(mesh):
    group = mesh.shape['data']
    tok_spec = P(('rep', 'data'), None)
    id_spec = P(('rep', 'data'))
    full_spec = P(None, None)
    own_spec = P('data', None, None)
    grad_spec = P(('rep', 'data'), None, None)

    def device_fn(x_loc, ids_loc, dy_loc, w_gate, w_up, w_down, a_gate, b_gate, a_up, b_up, a_down, b_down):
        tokens, dim = x_loc.shape
        n_local, _, rank = a_gate.shape
        hidden = w_gate.shape[1]
        width = n_local * rank
        scale = LORA_ALPHA / rank
        cap = ((3 * tokens + 8 * group - 1) // (8 * group)) * 8
        rows = group * cap
        steps = hidden // TILE

        def exchange(arr):
            return lax.all_to_all(arr, 'data', 0, 0, tiled=True)

        def as_rows(weight):
            return jnp.swapaxes(weight, 1, 2).reshape(width, weight.shape[1])

        ag, au, ad = as_rows(a_gate), as_rows(a_up), as_rows(a_down)
        bg, bu, bd = b_gate.reshape(width, hidden), b_up.reshape(width, hidden), b_down.reshape(width, dim)

        def arr(shape, dtype):
            return jax.ShapeDtypeStruct(shape, dtype)

        base = 2 * rows * dim * hidden
        lora = 2 * rows * width * hidden
        small = 2 * rows * width * dim
        chunks = dim // TILE
        any_spec = pl.BlockSpec(memory_space=pl.ANY)
        vmem_spec = pl.BlockSpec(memory_space=pltpu.VMEM)
        sem = pltpu.SemaphoreType.DMA
        x, dy, h, dg, du, dx, out, pack, pgt, put, qdt, pd, qg, qu = pl.pallas_call(
            functools.partial(layer_body, cap, n_local, rank, scale, mesh.axis_names),
            in_specs=[vmem_spec] + [any_spec] * 11,
            out_specs=[any_spec] * 6 + [vmem_spec] * 5 + [any_spec] * 3,
            out_shape=[arr((rows, dim), bf)] * 2 + [arr((rows, hidden), bf)] * 3 + [arr((rows, dim), bf), arr((tokens, dim), bf), arr((rows, tokens), bf)]
            + [arr((width, rows), bf)] * 3 + [arr((rows, width), bf)] * 3,
            scratch_shapes=[
                pltpu.VMEM((2, rows, hidden), f32),
                pltpu.VMEM((rows, dim), bf), pltpu.VMEM((rows, dim), bf), pltpu.VMEM((rows, dim), bf), pltpu.VMEM((rows, dim), bf),
                pltpu.VMEM((rows, dim), bf),
                pltpu.VMEM((group, 8, 128), f32), pltpu.VMEM((group, 8, 128), f32),
                pltpu.VMEM((8, TILE, dim), bf), pltpu.VMEM((2, 3, width, TILE), bf),
                pltpu.VMEM((rows, dim), f32), pltpu.VMEM((rows, width), f32), pltpu.VMEM((rows, width), f32),
                pltpu.VMEM((rows, width), bf), pltpu.VMEM((rows, width), bf),
                sem((chunks + 3, group)), sem((chunks + 3, group)), sem((8,)), sem((2, 3)), sem((dim // TILE, 2)), sem((2,)), sem((5,)),
            ],
            compiler_params=pltpu.CompilerParams(collective_id=0, has_side_effects=True, vmem_limit_bytes=67043328),
            cost_estimate=cost(6 * base + 6 * lora + 6 * small, 12 * dim * hidden),
            name='layer',
        )(ids_loc[None, :], x_loc, dy_loc, ag, au, bd, w_gate, w_up, w_down, bg, bu, ad)
        g_bg, g_bu, g_ad, g_ag, g_au, g_bd = pl.pallas_call(
            functools.partial(grads_body, scale),
            in_specs=[any_spec] * 11,
            out_specs=[any_spec] * 6,
            out_shape=[arr((width, hidden), f32)] * 3 + [arr((width, dim), f32)] * 3,
            scratch_shapes=[
                pltpu.VMEM((3, width, rows), bf), pltpu.VMEM((3, rows, width), bf), pltpu.VMEM((3, width, rows), bf), pltpu.VMEM((2, rows, dim), bf),
                pltpu.VMEM((DEEP, 3, rows, TILE), bf), pltpu.VMEM((DEEP, 3, width, TILE), f32),
                sem((3,)), sem((3,)), sem((2,)), sem((DEEP, 3)), sem((DEEP, 3)),
            ],
            compiler_params=pltpu.CompilerParams(vmem_limit_bytes=60 * 2 ** 20),
            cost_estimate=cost(3 * lora + 3 * small, 12 * width * hidden),
            name='adapter_grads',
        )(pgt, put, qdt, pd, qg, qu, x, dy, h, dg, du)

        def back(vals):
            return mm(pack, exchange(vals), 0, 0).astype(bf)

        def a_grad(vals):
            return jnp.swapaxes(vals.reshape(n_local, rank, vals.shape[1]), 1, 2)

        def b_grad(vals):
            return vals.reshape(n_local, rank, vals.shape[1])

        return out, back(dx), a_grad(g_ag), b_grad(g_bg), a_grad(g_au), b_grad(g_bu), a_grad(g_ad), b_grad(g_bd)

    return jax.shard_map(
        device_fn,
        mesh=mesh,
        in_specs=(tok_spec, id_spec, tok_spec, full_spec, full_spec, full_spec) + (own_spec,) * 6,
        out_specs=(tok_spec, tok_spec) + (grad_spec,) * 6,
        check_vma=False,
    )
```
